768 devices in a mesh: pair: 32 (over y, x), grow: 8 (over z_lo, core), gcol: 3 (over z_hi).
Axes of the slice: x: 4, y: 8, z: 12 (z_hi: 3, z_lo: 4; z = z_hi * 4 + z_lo), core: 2. Of those that a mesh axis runs over, the one named last changes fastest.
Arguments:
- valence: bfloat16 [16, 96, 9216], P(None, 'grow'), may hold values from -6 to 6
- conduction: bfloat16 [192, 96, 9216], P(('pair', 'gcol'), 'grow'), may hold values from -6 to 6
- val_energy: float32 [16], replicated, may hold values from -10 to -1
- cond_energy: float32 [192], replicated, may hold values from 1 to 20
- val_occupation: int32 [16], replicated, may hold values from 1 to 16
- gvectors: int32 [3, 3840], replicated, may hold values from -12 to 12, as said below
Outputs:
- chi_zero: float32 [7680, 7680], P(('pair', 'gcol'), 'grow')
The draws below stay inside these ranges and needn't reach their ends.
Inputs may be any that keep to these rules, and one draw needn't show every extreme that they name: gvectors holds 3840 distinct wave vectors; the first component lies in 1 .. 12, the other two in -12 .. 12.
All inputs are finite; a program needn't handle non-finite values.
Results may differ from the reference program's by a relative error of at most 0.02.
Values may be sent and summed in bfloat16 or wider, within the bound.
A program may use at most 64 MiB of HBM per device.

```python
import math
import jax
import jax.numpy as jnp
from jax import lax

N = 96
RAD = 12
KG = 3840
NV = 16
NCOND = 192
NPAIRS = 3072
N_GROW = 8


def draw_gvectors(key, part):
    extent = 2 * RAD + 1
    total_count = RAD * extent * extent
    chosen = jax.random.permutation(jax.random.fold_in(key, 11), total_count)[:KG]
    component_a = chosen // (extent * extent) + 1
    component_b = chosen // extent % extent - RAD
    component_c = chosen % extent - RAD
    return jnp.stack([component_a, component_b, component_c]).astype(jnp.int32)


def touch_ends(array, key, low, top_value):
    place = [jax.random.randint(jax.random.fold_in(key, axis), (), 0, length) for axis, length in enumerate(array.shape)]
    main_axis = array.shape.index(max(array.shape))
    neighbour = place[:main_axis] + [(place[main_axis] + 1) % array.shape[main_axis]] + place[main_axis + 1:]
    return array.at[tuple(place)].set(low).at[tuple(neighbour)].set(top_value)


def steps_of(rng, shape, pieces, low, top_value):
    def one(axis_at, parts):
        steps = jax.random.uniform(jax.random.fold_in(jax.random.fold_in(rng, 6), axis_at), (parts,), jnp.float32, low / len(pieces), top_value / len(pieces))
        return jnp.repeat(jnp.exp(steps), shape[axis_at] // parts).reshape((-1,) + (1,) * (len(shape) - axis_at - 1))

    level = one(*pieces[0])
    for cut in pieces[1:]:
        level = level * one(*cut)
    return level


def scatter_about(key, shape, deviation, reach, cuts=(), kind=jnp.bfloat16):
    gain = steps_of(key, shape, cuts, -0.22, 0.18) if cuts else 1.0
    array = jax.random.normal(key, shape, jnp.float32) * deviation * gain
    return jnp.minimum(jnp.maximum(array, -reach), reach).astype(kind)


def setup_inputs(seed: int = 0) -> dict:
    arg_keys = jax.random.split(jax.random.key(seed), 7)
    valence = scatter_about(arg_keys[0], (NV, N, N * N), 1.0, 6.0, ((1, 8),))
    conduction = scatter_about(arg_keys[1], (NCOND, N, N * N), 1.0, 6.0, ((0, 96), (1, 8)))
    val_energy = jnp.clip(jax.random.uniform(arg_keys[2], (NV,), jnp.float32, -10.0, -1.0), -10.0, -1.0)
    cond_energy = jnp.clip(jax.random.uniform(arg_keys[3], (NCOND,), jnp.float32, 1.0, 20.0), 1.0, 20.0)
    val_occupation = touch_ends(jax.random.randint(arg_keys[4], (NV,), 1, 17), jax.random.fold_in(arg_keys[4], 1), 1, 16).astype(jnp.int32)
    gvectors = draw_gvectors(jax.random.fold_in(arg_keys[6], 71), 0)
    return dict(valence=valence, conduction=conduction, val_energy=val_energy, cond_energy=cond_energy, val_occupation=val_occupation, gvectors=gvectors)


def wave_tables(positions, frequencies):
    phases = jnp.mod(positions[:, None] * frequencies[None, :], N).astype(jnp.float32) * (2.0 * math.pi / N)
    return (jnp.cos(phases), jnp.sin(phases))

def build_tables(x_positions):
    all_freq = jnp.arange(-RAD, RAD + 1, dtype=jnp.int32)
    pos_freq = jnp.arange(1, RAD + 1, dtype=jnp.int32)
    positions = jnp.arange(N, dtype=jnp.int32)
    cosine, sine_part = wave_tables(positions, all_freq)
    z_table = jnp.concatenate([cosine, sine_part], 1).astype(jnp.bfloat16)
    y_table = jnp.stack([jnp.stack([cosine, sine_part], 1), jnp.stack([-sine_part, cosine], 1)], 1).astype(jnp.bfloat16)
    x_cos, x_sin = wave_tables(x_positions, pos_freq)
    x_table = jnp.stack([jnp.stack([x_cos, -x_sin], 1), jnp.stack([-x_sin, -x_cos], 1)], 1).astype(jnp.bfloat16)
    return (z_table, y_table, x_table)

def band_transform(one_band, valence, z_table, y_table, x_table, flat_index):
    extent = 2 * RAD + 1
    planes = N // N_GROW
    density = valence * one_band[None]
    section_one = jnp.dot(density.reshape(-1, N), z_table, preferred_element_type=jnp.float32).astype(jnp.bfloat16)
    section_one = section_one.reshape(NV * N, N, 2, extent)
    second = jnp.einsum('ayik,yioj->aojk', section_one.astype(jnp.float32), y_table.astype(jnp.float32)).astype(jnp.bfloat16)
    second = second.reshape(NV, N_GROW, planes, 2, extent * extent)
    block_table = x_table.reshape(N_GROW, planes, 2, 2, RAD)
    blocks = jnp.einsum('pbxoq,bxosm->pbsmq', second.astype(jnp.float32), block_table.astype(jnp.float32))
    rounded = lax.optimization_barrier(blocks.astype(jnp.bfloat16))
    section_three = lax.optimization_barrier(jnp.sum(rounded.astype(jnp.float32), axis=1))
    section_three = section_three.reshape(NV, 2, RAD * extent * extent)
    picked = jnp.take(section_three, flat_index, axis=2)
    return picked.reshape(NV, 2 * KG)

def reference(valence, conduction, val_energy, cond_energy, val_occupation, gvectors):
    extent = 2 * RAD + 1
    z_table, y_table, x_table = build_tables(jnp.arange(N, dtype=jnp.int32))
    flat_index = (((gvectors[0] - 1) * extent + gvectors[1] + RAD) * extent + gvectors[2] + RAD).astype(jnp.int32)
    weight = val_occupation.astype(jnp.float32)[None, :] / (4.0 * (cond_energy[:, None] - val_energy[None, :]))
    factor = jnp.sqrt(weight) * (1.0 / N ** 1.5)

    def per_band(inputs):
        one_band, band_factor = inputs
        picked = band_transform(one_band, valence, z_table, y_table, x_table, flat_index)
        return (picked * band_factor[:, None]).astype(jnp.bfloat16)
    weighted = lax.map(per_band, (conduction, factor))
    flattened = weighted.reshape(-1, 2 * KG)
    chi_block = lax.dot_general(flattened, flattened, (((0,), (0,)), ((), ())), preferred_element_type=jnp.float32)
    return chi_block * (-1.0 / math.sqrt(NPAIRS))
```

```python
import functools
import math

import jax
import jax.numpy as jnp
import numpy as np
from jax import lax
from jax.experimental import pallas as pl
from jax.experimental.pallas import tpu as pltpu
from jax.sharding import Mesh
from jax.sharding import PartitionSpec as P

PAIR = ("pair_0", "pair_1")
PAIR_GCOL = ("pair_0", "pair_1", "gcol")

N=96; RAD=12; KG=3840; NV=16
PL=12
PART=1152
HALF=math.sqrt(0.5)

def lane_waves():
    j=np.zeros((4,128),np.int64); k=np.zeros((4,128),np.int64); used=np.zeros((4,2,128))
    for l in range(91):
        j[0,l],k[0,l]=(-8+8*(l//13),l%13) if l<39 else (-12+8*((l-39)//13),(l-39)%13)
        used[0,0 if l<39 else 1,l]=1
    for c in (1,2,3):
        for l in range(75):
            j[c,l],k[c,l]=c-8+8*(l//25),l%25-12
            used[c,:,l]=1
    return j,k,used

def phase_of(n): return 2*np.pi*np.mod(n,N)/N

def tables():
    j,k,used=lane_waves()
    z=np.arange(N); y=np.arange(12)
    kz=phase_of(z[None,:,None]*k[:2,None,:])
    z_tab=np.stack([np.cos(kz),np.sin(kz)],1).astype(np.float32)
    jy=phase_of(y[None,:,None]*j[:,None,:])
    y_tab=np.stack([np.cos(jy),np.sin(jy)],1)
    first=np.where(used[:,0,None,None,:]>0,y_tab,0.0)
    y_tab0=np.where(used[0,1,None,None,:]>0,y_tab[0],0.0)
    y_all=np.concatenate([first,y_tab0[None]],0).astype(np.float32)
    a=np.arange(16)
    X=np.arange(N).reshape(8,12)
    ax=phase_of(X[:,:,None]*a[None,None,:])
    x_tab=np.zeros((8,32,16),np.float32)
    x_tab[:,:12]=np.cos(ax); x_tab[:,16:28]=np.sin(ax)
    return z_tab,y_all,x_tab

def transform_body(grow, val, con, gvec, z_tab, y_tab, x_tab, out, vbuf, cbuf, tab, mixed, sec_re, sec_im, keys, sems):
    copies=[]
    for s in range(4):
        copies.append((pltpu.make_async_copy(val.at[pl.ds(3*s,3)],vbuf.at[pl.ds(3*s,3)],sems.at[s]),
                       pltpu.make_async_copy(con.at[pl.ds(3*s,3)],cbuf.at[pl.ds(3*s,3)],sems.at[4+s])))
    for pair in copies:
        for c in pair: c.start()
    def build(yp,_):
        row=pl.ds(pl.multiple_of(yp*N,32),N)
        for t in range(4):
            cz=z_tab[min(t,1),0]; sz=z_tab[min(t,1),1]
            cy=y_tab[t,0,pl.ds(yp,1)]; sy=y_tab[t,1,pl.ds(yp,1)]
            co=(cy*cz-sy*sz); si=(sy*cz+cy*sz)
            tab[t,row,0:128]=co.astype(jnp.bfloat16)
            tab[t,row,128:256]=si.astype(jnp.bfloat16)
            row2=pl.ds(pl.multiple_of(PART+yp*N,32),N)
            if t==0:
                cy=y_tab[4,0,pl.ds(yp,1)]; sy=y_tab[4,1,pl.ds(yp,1)]
                tab[t,row2,0:128]=(cy*cz-sy*sz).astype(jnp.bfloat16)
                tab[t,row2,128:256]=(sy*cz+cy*sz).astype(jnp.bfloat16)
            else:
                tab[t,row2,0:128]=(-si).astype(jnp.bfloat16)
                tab[t,row2,128:256]=co.astype(jnp.bfloat16)
        return 0
    lax.fori_loop(0,12,build,0)
    for b in range(4):
        lanes=pl.ds(960*b,960)
        a=gvec[0:1,lanes]; j=gvec[1:2,lanes]; k=gvec[2:3,lanes]
        j8=j&7
        flip=(j8>=5)|(((j8&3)==0)&((k<0)|((k==0)&(j<0))))
        j=jnp.where(flip,-j,j); k=jnp.where(flip,-k,k)
        c=j&7
        odd=128*c+25*((j+8-c)>>3)+k+12
        even=jnp.where(c==0,13*((j+8)>>3)+k,39+13*((j+12)>>3)+k)
        rho=jnp.where((c&3)==0,even,odd)
        keys[b,0:1,0:960]=rho
        keys[b,1:2,0:960]=a
        keys[b,2:3,0:960]=flip.astype(jnp.int32)
    def mix(x,_):
        for c in range(2):
            row=pl.ds(pl.multiple_of(x*32+16*c,16),16)
            for w in range(0,PART,384):
                d=[]
                for q in range(8):
                    lanes=pl.ds(q*PART+w,384)
                    d.append((vbuf[x,:,lanes]*cbuf[x,c:c+1,lanes]).astype(jnp.float32))
                a=[d[q]+d[q+4] for q in range(4)]
                m=[d[q]-d[q+4] for q in range(4)]
                p=(m[1]-m[3])*HALF; r=(m[1]+m[3])*HALF
                even=a[0]+a[2]; odd=a[1]+a[3]
                for t,(u,v) in enumerate([(even+odd,even-odd),(m[0]+p,m[2]+r),(a[0]-a[2],a[1]-a[3]),(m[0]-p,r-m[2])]):
                    mixed[t,row,w:w+384]=u.astype(jnp.bfloat16)
                    mixed[t,row,PART+w:PART+w+384]=v.astype(jnp.bfloat16)
        return 0
    for s in range(4):
        for c in copies[s]: c.wait()
        lax.fori_loop(3*s,3*s+3,mix,0)
    for t in range(4):
        both=jnp.dot(mixed[t],tab[t],preferred_element_type=jnp.float32)
        sec_re[:,128*t:128*(t+1)]=both[:,:128].astype(jnp.bfloat16)
        sec_im[:,128*t:128*(t+1)]=both[:,128:].astype(jnp.bfloat16)
    waves=x_tab[grow]
    def pick(b,_):
        for n0 in range(0,960,256):
            w=min(256,960-n0)
            lanes=pl.ds(n0,w)
            rho=keys[b,0:1,lanes]; a=keys[b,1:2,lanes]; sign=1.0-2.0*keys[b,2:3,lanes].astype(jnp.float32)
            hot=(lax.broadcasted_iota(jnp.int32,(512,w),0)==rho).astype(jnp.float32).astype(jnp.bfloat16)
            hot_a=(lax.broadcasted_iota(jnp.int32,(16,w),0)==a).astype(jnp.float32).astype(jnp.bfloat16)
            wave=jnp.dot(waves,hot_a,preferred_element_type=jnp.float32)
            re=jnp.dot(sec_re[...],hot,preferred_element_type=jnp.float32)
            im=jnp.dot(sec_im[...],hot,preferred_element_type=jnp.float32)
            tot_re=jnp.zeros((32,w),jnp.float32); tot_im=jnp.zeros((32,w),jnp.float32)
            for x in range(PL):
                co=wave[x:x+1]; si=wave[16+x:17+x]
                gr=re[32*x:32*x+32]; gi=im[32*x:32*x+32]
                tot_re+=co*gr-(si*sign)*gi
                tot_im+=si*gr+(co*sign)*gi
            out[b,:,lanes]=tot_re.astype(out.dtype)
            out[4+b,:,lanes]=(-tot_im).astype(out.dtype)
        return 0
    lax.fori_loop(0,4,pick,0)

def transform_scratch():
    return [pltpu.VMEM((PL,NV,9216),jnp.bfloat16), pltpu.VMEM((PL,2,9216),jnp.bfloat16),
        pltpu.VMEM((4,2*PART,256),jnp.bfloat16), pltpu.VMEM((4,384,2*PART),jnp.bfloat16),
        pltpu.VMEM((384,512),jnp.bfloat16), pltpu.VMEM((384,512),jnp.bfloat16),
        pltpu.VMEM((4,8,1024),jnp.int32), pltpu.SemaphoreType.DMA((8,))]


def kernel(*refs):
    transform_body(lax.axis_index("grow"), *refs)

def partial_sums(valence, conduction, gvectors):
    z_tab, y_tab, x_tab = tables()
    return pl.pallas_call(
        kernel,
        out_shape=jax.ShapeDtypeStruct((8, 32, 960), jnp.bfloat16),
        in_specs=[pl.BlockSpec(memory_space=pl.ANY)] * 2
        + [pl.BlockSpec(memory_space=pltpu.VMEM)] * 4,
        out_specs=pl.BlockSpec(memory_space=pltpu.VMEM),
        scratch_shapes=transform_scratch(),
        compiler_params=pltpu.CompilerParams(vmem_limit_bytes=48 * 2**20),
        name="transform",
    )(valence.transpose(1, 0, 2), conduction.transpose(1, 0, 2), gvectors,
      jnp.asarray(z_tab), jnp.asarray(y_tab), jnp.asarray(x_tab, jnp.bfloat16))

def in_blocks(shard, dim, size):
    dims = shard.shape
    parts = shard.reshape(*dims[:dim], size, dims[dim] // size, *dims[dim + 1 :])
    return jnp.moveaxis(parts, dim, 0)


def sent_and_summed(shard, axis, dim):
    parts = in_blocks(shard, dim, lax.axis_size(axis))
    arrived = lax.all_to_all(parts, axis, split_axis=0, concat_axis=0, tiled=True)
    return arrived.astype(jnp.float32).sum(axis=0)


def sent_to_all(shard, axis):
    copies = jnp.broadcast_to(shard, (lax.axis_size(axis), *shard.shape))
    return lax.all_to_all(copies, axis, split_axis=0, concat_axis=0, tiled=True)


def in_order(parts, dim):
    parts = jnp.moveaxis(parts, 0, dim)
    dims = parts.shape
    return parts.reshape(*dims[:dim], dims[dim] * dims[dim + 1], *dims[dim + 2 :])


def collect(shard, axis, dim):
    parts = sent_to_all(shard, axis)
    return in_order(parts, dim)


def gathered_by_axis(shard, axes, dim):
    for axis in reversed(axes):
        shard = lax.all_gather(shard, axis, axis=dim, tiled=True)
    return shard


def pair_product(left_rows, right_rows):
    return lax.dot_general(
        left_rows, right_rows, (((0,), (0,)), ((), ())), preferred_element_type=jnp.float32
    )


def body(valence, conduction, val_energy, cond_energy, val_occupation, gvectors):
    pair_count = lax.axis_size(PAIR)
    gcol_count = lax.axis_size("gcol")
    cond_bands = conduction.shape[0]
    local_pairs = cond_bands * NV
    parts = partial_sums(valence, conduction, gvectors)
    arrived = lax.all_to_all(parts, "grow", split_axis=0, concat_axis=0, tiled=True)
    summed = arrived.astype(jnp.float32).sum(axis=0)
    first_band = (lax.axis_index(PAIR) * gcol_count + lax.axis_index("gcol")) * cond_bands
    own_energy = lax.dynamic_slice_in_dim(cond_energy, first_band, cond_bands, 0)
    weight = val_occupation.astype(jnp.float32)[None, :] / (
        4.0 * (own_energy[:, None] - val_energy[None, :])
    )
    factor = (jnp.sqrt(weight) * (1.0 / N**1.5)).reshape(local_pairs, 1)
    weighted = (summed * factor).astype(jnp.bfloat16)
    prefactor = -1.0 / math.sqrt(pair_count * gcol_count * local_pairs)
    full_rows = collect(weighted, "grow", 1)
    row_part = lax.all_to_all(full_rows, PAIR, split_axis=1, concat_axis=0, tiled=True)
    partial_value = pair_product(row_part, gathered_by_axis(weighted, PAIR, 0))
    return sent_and_summed((partial_value * prefactor).astype(jnp.bfloat16), "gcol", 0)


def solution(mesh):
    finer = Mesh(
        mesh.devices.reshape(8, 4, mesh.shape["grow"], mesh.shape["gcol"]),
        ("pair_0", "pair_1", "grow", "gcol"),
    )
    placed = (P(None, "grow", None), P(PAIR_GCOL, "grow", None), P(), P(), P(), P())
    return jax.shard_map(
        body, mesh=finer, in_specs=placed, out_specs=P(PAIR_GCOL, "grow"), check_vma=False
    )
```

```python
import functools
import math

import jax
import jax.numpy as jnp
import numpy as np
from jax import lax
from jax.experimental import pallas as pl
from jax.experimental.pallas import tpu as pltpu
from jax.sharding import Mesh
from jax.sharding import PartitionSpec as P

N=96; RAD=12; KG=3840; NV=16
PL=12
PART=1152
HALF=math.sqrt(0.5)

def lane_waves():
    j=np.zeros((4,128),np.int64); k=np.zeros((4,128),np.int64); used=np.zeros((4,2,128))
    for l in range(91):
        j[0,l],k[0,l]=(-8+8*(l//13),l%13) if l<39 else (-12+8*((l-39)//13),(l-39)%13)
        used[0,0 if l<39 else 1,l]=1
    for c in (1,2,3):
        for l in range(75):
            j[c,l],k[c,l]=c-8+8*(l//25),l%25-12
            used[c,:,l]=1
    return j,k,used

def phase_of(n): return 2*np.pi*np.mod(n,N)/N

def tables():
    j,k,used=lane_waves()
    z=np.arange(N); y=np.arange(12)
    kz=phase_of(z[None,:,None]*k[:2,None,:])
    z_tab=np.stack([np.cos(kz),np.sin(kz)],1).astype(np.float32)
    jy=phase_of(y[None,:,None]*j[:,None,:])
    y_tab=np.stack([np.cos(jy),np.sin(jy)],1)
    first=np.where(used[:,0,None,None,:]>0,y_tab,0.0)
    y_tab0=np.where(used[0,1,None,None,:]>0,y_tab[0],0.0)
    y_all=np.concatenate([first,y_tab0[None]],0).astype(np.float32)
    a=np.arange(16)
    X=np.arange(N).reshape(8,12)
    ax=phase_of(X[:,:,None]*a[None,None,:])
    x_tab=np.zeros((8,32,16),np.float32)
    x_tab[:,:12]=np.cos(ax); x_tab[:,16:28]=np.sin(ax)
    return z_tab,y_all,x_tab

def transform_body(val, con, gvec_in, z_in, y_in, x_in, out, vbuf, cbuf, gvec, z_tab, y_tab, x_tab, tab, mixed, sec_re, sec_im, keys, sems):
    grow=2*lax.axis_index("zl")+lax.axis_index("core")
    small=[pltpu.make_async_copy(a,b,sems.at[8+i]) for i,(a,b) in enumerate([(z_in,z_tab),(y_in,y_tab),(gvec_in,gvec),(x_in.at[grow],x_tab)])]
    for c in small: c.start()
    copies=[]
    for s in range(4):
        copies.append((pltpu.make_async_copy(val.at[pl.ds(3*s,3)],vbuf.at[pl.ds(3*s,3)],sems.at[s]),
                       pltpu.make_async_copy(con.at[pl.ds(3*s,3)],cbuf.at[pl.ds(3*s,3)],sems.at[4+s])))
    for pair in copies:
        for c in pair: c.start()
    for c in small: c.wait()
    def build(yp,_):
        row=pl.ds(pl.multiple_of(yp*N,32),N)
        for t in range(4):
            cz=z_tab[min(t,1),0]; sz=z_tab[min(t,1),1]
            cy=y_tab[t,0,pl.ds(yp,1)]; sy=y_tab[t,1,pl.ds(yp,1)]
            co=(cy*cz-sy*sz); si=(sy*cz+cy*sz)
            tab[t,row,0:128]=co.astype(jnp.bfloat16)
            tab[t,row,128:256]=si.astype(jnp.bfloat16)
            row2=pl.ds(pl.multiple_of(PART+yp*N,32),N)
            if t==0:
                cy=y_tab[4,0,pl.ds(yp,1)]; sy=y_tab[4,1,pl.ds(yp,1)]
                tab[t,row2,0:128]=(cy*cz-sy*sz).astype(jnp.bfloat16)
                tab[t,row2,128:256]=(sy*cz+cy*sz).astype(jnp.bfloat16)
            else:
                tab[t,row2,0:128]=(-si).astype(jnp.bfloat16)
                tab[t,row2,128:256]=co.astype(jnp.bfloat16)
        return 0
    lax.fori_loop(0,12,build,0)
    keys[...] = jnp.zeros_like(keys)
    for b in range(16):
        lanes=pl.ds(240*b,240)
        a=gvec[0:1,lanes]; j=gvec[1:2,lanes]; k=gvec[2:3,lanes]
        j8=j&7
        flip=(j8>=5)|(((j8&3)==0)&((k<0)|((k==0)&(j<0))))
        j=jnp.where(flip,-j,j); k=jnp.where(flip,-k,k)
        c=j&7
        odd=128*c+25*((j+8-c)>>3)+k+12
        even=jnp.where(c==0,13*((j+8)>>3)+k,39+13*((j+12)>>3)+k)
        lanes=pl.ds(256*(b%4),240)
        keys[b//4,0:1,lanes]=jnp.where((c&3)==0,even,odd)
        keys[b//4,1:2,lanes]=a
        keys[b//4,2:3,lanes]=flip.astype(jnp.int32)
    def mix(x,_):
        for c in range(2):
            row=pl.ds(pl.multiple_of(x*32+16*c,16),16)
            for w in range(0,PART,384):
                d=[]
                for q in range(8):
                    lanes=pl.ds(q*PART+w,384)
                    d.append((vbuf[x,:,lanes]*cbuf[x,c:c+1,lanes]).astype(jnp.float32))
                a=[d[q]+d[q+4] for q in range(4)]
                m=[d[q]-d[q+4] for q in range(4)]
                p=(m[1]-m[3])*HALF; r=(m[1]+m[3])*HALF
                even=a[0]+a[2]; odd=a[1]+a[3]
                for t,(u,v) in enumerate([(even+odd,even-odd),(m[0]+p,m[2]+r),(a[0]-a[2],a[1]-a[3]),(m[0]-p,r-m[2])]):
                    mixed[t,row,w:w+384]=u.astype(jnp.bfloat16)
                    mixed[t,row,PART+w:PART+w+384]=v.astype(jnp.bfloat16)
        return 0
    for s in range(4):
        for c in copies[s]: c.wait()
        lax.fori_loop(3*s,3*s+3,mix,0)
    for t in range(4):
        both=jnp.dot(mixed[t],tab[t],preferred_element_type=jnp.float32)
        sec_re[:,128*t:128*(t+1)]=both[:,:128].astype(jnp.bfloat16)
        sec_im[:,128*t:128*(t+1)]=both[:,128:].astype(jnp.bfloat16)
    waves=x_tab[...]
    def pick(b,_):
        for n0 in range(0,1024,256):
            w=256
            lanes=pl.ds(n0,w)
            rho=keys[b,0:1,lanes]; a=keys[b,1:2,lanes]; sign=1.0-2.0*keys[b,2:3,lanes].astype(jnp.float32)
            hot=(lax.broadcasted_iota(jnp.int32,(512,w),0)==rho).astype(jnp.float32).astype(jnp.bfloat16)
            hot_a=(lax.broadcasted_iota(jnp.int32,(16,w),0)==a).astype(jnp.float32).astype(jnp.bfloat16)
            wave=jnp.dot(waves,hot_a,preferred_element_type=jnp.float32)
            re=jnp.dot(sec_re[...],hot,preferred_element_type=jnp.float32)
            im=jnp.dot(sec_im[...],hot,preferred_element_type=jnp.float32)
            tot_re=jnp.zeros((32,w),jnp.float32); tot_im=jnp.zeros((32,w),jnp.float32)
            for x in range(PL):
                co=wave[x:x+1]; si=wave[16+x:17+x]
                gr=re[32*x:32*x+32]; gi=im[32*x:32*x+32]
                tot_re+=co*gr-(si*sign)*gi
                tot_im+=si*gr+(co*sign)*gi
            out[b//2,lax.rem(b,2),:,lanes]=tot_re.astype(out.dtype)
            out[2+b//2,lax.rem(b,2),:,lanes]=(-tot_im).astype(out.dtype)
        return 0
    lax.fori_loop(0,4,pick,0)

def transform_scratch():
    return [pltpu.VMEM((PL,NV,9216),jnp.bfloat16), pltpu.VMEM((PL,2,9216),jnp.bfloat16),
        pltpu.VMEM((3,KG),jnp.int32), pltpu.VMEM((2,2,96,128),jnp.float32), pltpu.VMEM((5,2,12,128),jnp.float32), pltpu.VMEM((32,16),jnp.bfloat16),
        pltpu.VMEM((4,2*PART,256),jnp.bfloat16), pltpu.VMEM((4,384,2*PART),jnp.bfloat16),
        pltpu.VMEM((384,512),jnp.bfloat16), pltpu.VMEM((384,512),jnp.bfloat16),
        pltpu.VMEM((4,8,1024),jnp.int32), pltpu.SemaphoreType.DMA((12,))]


def partial_sums(valence, conduction, gvectors):
    z_tab, y_tab, x_tab = tables()
    return pl.pallas_call(
        transform_body,
        out_shape=jax.ShapeDtypeStruct((4, 2, 32, 1024), jnp.bfloat16),
        in_specs=[pl.BlockSpec(memory_space=pl.ANY)] * 6,
        out_specs=pl.BlockSpec(memory_space=pltpu.VMEM),
        scratch_shapes=transform_scratch(),
        compiler_params=pltpu.CompilerParams(vmem_limit_bytes=48 * 2**20),
        name="transform",
    )(valence.transpose(1, 0, 2), conduction.transpose(1, 0, 2), gvectors,
      jnp.asarray(z_tab), jnp.asarray(y_tab), jnp.asarray(x_tab, jnp.bfloat16))

MESH_AXES = ("y", "x", "zl", "core", "zh")
SIDE = pl.DeviceIdType.MESH
SUB = 256
WIDE = 4 * SUB


def turned(axis, step):
    size = lax.axis_size(axis)
    return lax.rem(lax.axis_index(axis) + step % size, size)


def remote(src, dst, send_sem, recv_sem, target):
    return pltpu.make_async_remote_copy(src_ref=src, dst_ref=dst, send_sem=send_sem, recv_sem=recv_sem,
                                        device_id=target, device_id_type=SIDE)


def pair_factor(val_energy, cond_energy, occupation):
    first = ((lax.axis_index("y") * 4 + lax.axis_index("x")) * 3 + lax.axis_index("zh")) * 2
    row = lax.broadcasted_iota(jnp.int32, (32, 16), 0)
    at_v = lax.broadcasted_iota(jnp.int32, (32, 16), 1) == (row & 15)
    ev = jnp.sum(jnp.where(at_v, val_energy, 0.0), axis=1, keepdims=True)
    occ = jnp.sum(jnp.where(at_v, occupation.astype(jnp.float32), 0.0), axis=1, keepdims=True)
    row = lax.broadcasted_iota(jnp.int32, (32, 192), 0)
    at_c = lax.broadcasted_iota(jnp.int32, (32, 192), 1) == first + (row >> 4)
    ec = jnp.sum(jnp.where(at_c, cond_energy, 0.0), axis=1, keepdims=True)
    return jnp.sqrt(occ / (4.0 * (ec - ev))) * (1.0 / N**1.5)


def exchange_body(parts, val_energy, cond_energy, occupation, out,
                  core_in, z_out, z_in, cols, rows, x_out, x_in,
                  core_sems, z_sems, zh_sems, y_sems, row_sems, row_out_sems, x_sems):
    y, x, zl, core, zh = (lax.axis_index(a) for a in MESH_AXES)
    barrier = pltpu.get_barrier_semaphore()
    partners = ([{"core": 1 - core}] + [{"zl": turned("zl", k)} for k in (1, 2, 3)]
                + [{"zh": turned("zh", k)} for k in (1, 2)] + [{"y": turned("y", k)} for k in (1, 7)]
                + [{"x": turned("x", k)} for k in (1, 2, 3)])
    for target in partners:
        pl.semaphore_signal(barrier, inc=1, device_id=target, device_id_type=SIDE)
    pl.semaphore_wait(barrier, len(partners))

    other = {"core": 1 - core}
    swaps = []
    for k in (2, 1, 3, 0):
        z = turned("zl", k)
        swaps.append((k, z, remote(parts.at[z, 1 - core], core_in.at[k], core_sems.at[0, k], core_sems.at[1, k], other)))
    for _, _, c in swaps:
        c.start()
    z_copies = []
    for k, z, c in swaps:
        c.wait_recv()
        both = parts[z, core].astype(jnp.float32) + core_in[k].astype(jnp.float32)
        if k:
            z_out[k - 1] = both.astype(jnp.bfloat16)
            c2 = remote(z_out.at[k - 1], z_in.at[k - 1], z_sems.at[0, k - 1], z_sems.at[1, k - 1], {"zl": z})
            c2.start()
            z_copies.append(c2)
        else:
            total = both
    factor = pair_factor(val_energy[...], cond_energy[...], occupation[...])
    for c in z_copies:
        c.wait_recv()
    for k in range(3):
        total = total + z_in[k].astype(jnp.float32)
    mine = zh * 8 + y
    cols[mine] = (total * factor).astype(jnp.bfloat16)

    zh_copies = []
    for k in (1, 2):
        c = remote(cols.at[mine], cols.at[mine], zh_sems.at[0, k - 1], zh_sems.at[1, k - 1], {"zh": turned("zh", k)})
        c.start()
        zh_copies.append(c)

    plane = 2 * zl + core
    home = y // 2
    on_chain = core == lax.rem(y, 2)
    source = plane == y

    def slot(t, step):
        return turned("zh", -t) * 8 + turned("y", step)

    def pick_rows(s):
        here = lax.broadcasted_iota(jnp.int32, (SUB, 128), 0)
        there = lax.broadcasted_iota(jnp.int32, (SUB, 128), 1)
        pick = ((here == there + 80 * zh) & (there < 80)).astype(jnp.float32).astype(jnp.bfloat16)
        for q in range(4):
            cut = jnp.dot(cols[s, :, SUB * q : SUB * (q + 1)], pick, preferred_element_type=jnp.float32)
            rows[s, :, 128 * q : 128 * (q + 1)] = cut.astype(jnp.bfloat16)

    def pass_rows(t, step):
        n = t * 8 + step % 8
        s = slot(t, step)

        def send(i, target):
            remote(rows.at[s], rows.at[s], row_out_sems.at[n, i], row_sems.at[n], target).start()

        @pl.when(source)
        def _():
            pick_rows(s)

        @pl.when(jnp.logical_not(source))
        def _():
            remote(rows.at[s], rows.at[s], row_out_sems.at[n, 0], row_sems.at[n], other).wait_recv()

        @pl.when(on_chain)
        def _():
            send(0, other)

        @pl.when(on_chain & (zl >= home) & (zl < 3))
        def _():
            send(1, {"zl": lax.rem(zl + 1, 4)})

        @pl.when(on_chain & (zl <= home) & (zl > 0))
        def _():
            send(2, {"zl": lax.rem(zl + 3, 4)})

    def ring(t, way, hop):
        s = slot(t, -way * (hop - 1))
        d = 0 if way == 1 else 1
        n = (t * 4 + hop - 1) * 2 + d
        half = pl.ds(0, 32) if hop < 4 else pl.ds(16 * d, 16)
        return remote(cols.at[s, half], cols.at[s, half], y_sems.at[0, n], y_sems.at[1, n], {"y": turned("y", way)})

    def landed(t, way, hop):
        s = slot(t, -way * hop)
        d = 0 if way == 1 else 1
        n = (t * 4 + hop - 1) * 2 + d
        half = pl.ds(0, 32) if hop < 4 else pl.ds(16 * d, 16)
        remote(cols.at[s, half], cols.at[s, half], y_sems.at[0, n], y_sems.at[1, n], {"y": turned("y", way)}).wait_recv()

    def start(t, hop):
        ring(t, 1, hop).start()
        ring(t, -1, hop).start()

    start(0, 1)
    pass_rows(0, 0)
    for hop in (1, 2, 3):
        landed(0, 1, hop)
        ring(0, 1, hop + 1).start()
        landed(0, -1, hop)
        ring(0, -1, hop + 1).start()
        pass_rows(0, -hop)
        pass_rows(0, hop)
    for t in (1, 2):
        zh_copies[t - 1].wait_recv()
        start(t, 1)
    for t in (1, 2):
        pass_rows(t, 0)
    landed(0, 1, 4)
    landed(0, -1, 4)
    pass_rows(0, 4)
    for hop in (1, 2, 3):
        for t in (1, 2):
            landed(t, 1, hop)
            ring(t, 1, hop + 1).start()
            landed(t, -1, hop)
            ring(t, -1, hop + 1).start()
        for t in (1, 2):
            pass_rows(t, -hop)
            pass_rows(t, hop)
    for t in (1, 2):
        landed(t, 1, 4)
        landed(t, -1, 4)
        pass_rows(t, 4)

    right = cols[...].reshape(768, WIDE)
    x_copies = []
    for k in (2, 1, 3, 0):
        q = turned("x", k)
        left = rows[:, :, pl.ds(pl.multiple_of(128 * q, 128), 128)].reshape(768, 128)
        block = lax.dot_general(left, right, (((0,), (0,)), ((), ())), preferred_element_type=jnp.float32)
        if k:
            x_out[k - 1] = block[:80].astype(jnp.bfloat16)
            c = remote(x_out.at[k - 1], x_in.at[k - 1], x_sems.at[0, k - 1], x_sems.at[1, k - 1], {"x": q})
            c.start()
            x_copies.append(c)
        else:
            total = block[:80]
    for c in x_copies:
        c.wait_recv()
    for k in range(3):
        total = total + x_in[k].astype(jnp.float32)
    out[...] = total * (-1.0 / math.sqrt(3072))

    for _, _, c in swaps:
        c.wait_send()
    for c in z_copies + zh_copies + x_copies:
        c.wait_send()
    for t in range(3):
        for hop in (1, 2, 3, 4):
            ring(t, 1, hop).wait_send()
            ring(t, -1, hop).wait_send()

    def rows_left(i):
        for t in range(3):
            for step in range(8):
                n = t * 8 + step
                s = slot(t, step)
                remote(rows.at[s], rows.at[s], row_out_sems.at[n, i], row_sems.at[n], other).wait_send()

    @pl.when(on_chain)
    def _():
        rows_left(0)

    @pl.when(on_chain & (zl >= home) & (zl < 3))
    def _():
        rows_left(1)

    @pl.when(on_chain & (zl <= home) & (zl > 0))
    def _():
        rows_left(2)


def exchange_scratch():
    dma = pltpu.SemaphoreType.DMA
    return [
        pltpu.VMEM((4, 32, WIDE), jnp.bfloat16),
        pltpu.VMEM((3, 32, WIDE), jnp.bfloat16),
        pltpu.VMEM((3, 32, WIDE), jnp.bfloat16),
        pltpu.VMEM((24, 32, WIDE), jnp.bfloat16),
        pltpu.VMEM((24, 32, 512), jnp.bfloat16),
        pltpu.VMEM((3, 80, WIDE), jnp.bfloat16),
        pltpu.VMEM((3, 80, WIDE), jnp.bfloat16),
        dma((2, 4)), dma((2, 3)), dma((2, 2)), dma((2, 24)), dma((24,)), dma((24, 3)), dma((2, 3)),
    ]


def exchange(parts, val_energy, cond_energy, occupation):
    return pl.pallas_call(
        exchange_body,
        out_shape=jax.ShapeDtypeStruct((80, WIDE), jnp.float32),
        in_specs=[pl.BlockSpec(memory_space=pltpu.VMEM)] * 4,
        out_specs=pl.BlockSpec(memory_space=pltpu.VMEM),
        scratch_shapes=exchange_scratch(),
        compiler_params=pltpu.CompilerParams(collective_id=0, has_side_effects=True, vmem_limit_bytes=32 * 2**20),
        name="exchange",
    )(parts, val_energy, cond_energy, occupation)


def body(valence, conduction, val_energy, cond_energy, val_occupation, gvectors):
    parts = partial_sums(valence, conduction, gvectors)
    chi = exchange(parts, val_energy.reshape(1, 16), cond_energy.reshape(1, 192), val_occupation.reshape(1, 16))
    return jnp.concatenate([chi[:, SUB * q : SUB * q + 240] for q in range(4)], axis=1)


def solution(mesh):
    finer = Mesh(mesh.devices.reshape(8, 4, 4, 2, 3), MESH_AXES)
    grow = ("zl", "core")
    bands = ("y", "x", "zh")
    placed = (P(None, grow, None), P(bands, grow, None), P(), P(), P(), P())
    return jax.shard_map(body, mesh=finer, in_specs=placed, out_specs=P(bands, grow), check_vma=False)
```

```python
import functools
import math

import jax
import jax.numpy as jnp
import numpy as np
from jax import lax
from jax.experimental import pallas as pl
from jax.experimental.pallas import tpu as pltpu
from jax.sharding import Mesh
from jax.sharding import PartitionSpec as P

N=96; RAD=12; KG=3840; NV=16
PL=12
PART=1152
HALF=math.sqrt(0.5)

def lane_waves():
    j=np.zeros((4,128),np.int64); k=np.zeros((4,128),np.int64); used=np.zeros((4,2,128))
    for l in range(91):
        j[0,l],k[0,l]=(-8+8*(l//13),l%13) if l<39 else (-12+8*((l-39)//13),(l-39)%13)
        used[0,0 if l<39 else 1,l]=1
    for c in (1,2,3):
        for l in range(75):
            j[c,l],k[c,l]=c-8+8*(l//25),l%25-12
            used[c,:,l]=1
    return j,k,used

def phase_of(n): return 2*np.pi*np.mod(n,N)/N

def tables():
    j,k,used=lane_waves()
    z=np.arange(N); y=np.arange(12)
    kz=phase_of(z[None,:,None]*k[:2,None,:])
    z_tab=np.stack([np.cos(kz),np.sin(kz)],1).astype(np.float32)
    jy=phase_of(y[None,:,None]*j[:,None,:])
    y_tab=np.stack([np.cos(jy),np.sin(jy)],1)
    first=np.where(used[:,0,None,None,:]>0,y_tab,0.0)
    y_tab0=np.where(used[0,1,None,None,:]>0,y_tab[0],0.0)
    y_all=np.concatenate([first,y_tab0[None]],0).astype(np.float32)
    a=np.arange(16)
    X=np.arange(N).reshape(8,12)
    ax=phase_of(X[:,:,None]*a[None,None,:])
    x_tab=np.zeros((8,32,16),np.float32)
    x_tab[:,:12]=np.cos(ax); x_tab[:,16:28]=np.sin(ax)
    return z_tab,y_all,x_tab

def transform_body(val, con, gvec_in, z_in, y_in, x_in, out, vbuf, cbuf, gvec, z_tab, y_tab, x_tab, tab, mixed, sec_re, sec_im, keys, sems):
    grow=2*lax.axis_index("zl")+lax.axis_index("core")
    small=[pltpu.make_async_copy(a,b,sems.at[8+i]) for i,(a,b) in enumerate([(z_in,z_tab),(y_in,y_tab),(gvec_in,gvec),(x_in.at[grow],x_tab)])]
    for c in small: c.start()
    copies=[]
    for s in range(4):
        copies.append((pltpu.make_async_copy(val.at[pl.ds(3*s,3)],vbuf.at[pl.ds(3*s,3)],sems.at[s]),
                       pltpu.make_async_copy(con.at[pl.ds(3*s,3)],cbuf.at[pl.ds(3*s,3)],sems.at[4+s])))
    for pair in copies:
        for c in pair: c.start()
    for c in small: c.wait()
    def build(yp,_):
        row=pl.ds(pl.multiple_of(yp*N,32),N)
        for t in range(4):
            cz=z_tab[min(t,1),0]; sz=z_tab[min(t,1),1]
            cy=y_tab[t,0,pl.ds(yp,1)]; sy=y_tab[t,1,pl.ds(yp,1)]
            co=(cy*cz-sy*sz); si=(sy*cz+cy*sz)
            tab[t,row,0:128]=co.astype(jnp.bfloat16)
            tab[t,row,128:256]=si.astype(jnp.bfloat16)
            row2=pl.ds(pl.multiple_of(PART+yp*N,32),N)
            if t==0:
                cy=y_tab[4,0,pl.ds(yp,1)]; sy=y_tab[4,1,pl.ds(yp,1)]
                tab[t,row2,0:128]=(cy*cz-sy*sz).astype(jnp.bfloat16)
                tab[t,row2,128:256]=(sy*cz+cy*sz).astype(jnp.bfloat16)
            else:
                tab[t,row2,0:128]=(-si).astype(jnp.bfloat16)
                tab[t,row2,128:256]=co.astype(jnp.bfloat16)
        return 0
    lax.fori_loop(0,12,build,0)
    keys[...] = jnp.zeros_like(keys)
    for b in range(16):
        lanes=pl.ds(240*b,240)
        a=gvec[0:1,lanes]; j=gvec[1:2,lanes]; k=gvec[2:3,lanes]
        j8=j&7
        flip=(j8>=5)|(((j8&3)==0)&((k<0)|((k==0)&(j<0))))
        j=jnp.where(flip,-j,j); k=jnp.where(flip,-k,k)
        c=j&7
        odd=128*c+25*((j+8-c)>>3)+k+12
        even=jnp.where(c==0,13*((j+8)>>3)+k,39+13*((j+12)>>3)+k)
        lanes=pl.ds(256*(b%4),240)
        keys[b//4,0:1,lanes]=jnp.where((c&3)==0,even,odd)
        keys[b//4,1:2,lanes]=a
        keys[b//4,2:3,lanes]=flip.astype(jnp.int32)
    def mix(x,_):
        for c in range(2):
            row=pl.ds(pl.multiple_of(x*32+16*c,16),16)
            for w in range(0,PART,384):
                d=[]
                for q in range(8):
                    lanes=pl.ds(q*PART+w,384)
                    d.append((vbuf[x,:,lanes]*cbuf[x,c:c+1,lanes]).astype(jnp.float32))
                a=[d[q]+d[q+4] for q in range(4)]
                m=[d[q]-d[q+4] for q in range(4)]
                p=(m[1]-m[3])*HALF; r=(m[1]+m[3])*HALF
                even=a[0]+a[2]; odd=a[1]+a[3]
                for t,(u,v) in enumerate([(even+odd,even-odd),(m[0]+p,m[2]+r),(a[0]-a[2],a[1]-a[3]),(m[0]-p,r-m[2])]):
                    mixed[t,row,w:w+384]=u.astype(jnp.bfloat16)
                    mixed[t,row,PART+w:PART+w+384]=v.astype(jnp.bfloat16)
        return 0
    for s in range(4):
        for c in copies[s]: c.wait()
        lax.fori_loop(3*s,3*s+3,mix,0)
    for t in range(4):
        both=jnp.dot(mixed[t],tab[t],preferred_element_type=jnp.float32)
        sec_re[:,128*t:128*(t+1)]=both[:,:128].astype(jnp.bfloat16)
        sec_im[:,128*t:128*(t+1)]=both[:,128:].astype(jnp.bfloat16)
    waves=x_tab[...]
    def pick(b,_):
        for n0 in range(0,1024,256):
            w=256
            lanes=pl.ds(n0,w)
            rho=keys[b,0:1,lanes]; a=keys[b,1:2,lanes]; sign=1.0-2.0*keys[b,2:3,lanes].astype(jnp.float32)
            hot=(lax.broadcasted_iota(jnp.int32,(512,w),0)==rho).astype(jnp.float32).astype(jnp.bfloat16)
            hot_a=(lax.broadcasted_iota(jnp.int32,(16,w),0)==a).astype(jnp.float32).astype(jnp.bfloat16)
            wave=jnp.dot(waves,hot_a,preferred_element_type=jnp.float32)
            re=jnp.dot(sec_re[...],hot,preferred_element_type=jnp.float32)
            im=jnp.dot(sec_im[...],hot,preferred_element_type=jnp.float32)
            tot_re=jnp.zeros((32,w),jnp.float32); tot_im=jnp.zeros((32,w),jnp.float32)
            for x in range(PL):
                co=wave[x:x+1]; si=wave[16+x:17+x]
                gr=re[32*x:32*x+32]; gi=im[32*x:32*x+32]
                tot_re+=co*gr-(si*sign)*gi
                tot_im+=si*gr+(co*sign)*gi
            out[b//2,lax.rem(b,2),:,lanes]=tot_re.astype(out.dtype)
            out[2+b//2,lax.rem(b,2),:,lanes]=(-tot_im).astype(out.dtype)
        return 0
    lax.fori_loop(0,4,pick,0)

def transform_scratch():
    return [pltpu.VMEM((PL,NV,9216),jnp.bfloat16), pltpu.VMEM((PL,2,9216),jnp.bfloat16),
        pltpu.VMEM((3,KG),jnp.int32), pltpu.VMEM((2,2,96,128),jnp.float32), pltpu.VMEM((5,2,12,128),jnp.float32), pltpu.VMEM((32,16),jnp.bfloat16),
        pltpu.VMEM((4,2*PART,256),jnp.bfloat16), pltpu.VMEM((4,384,2*PART),jnp.bfloat16),
        pltpu.VMEM((384,512),jnp.bfloat16), pltpu.VMEM((384,512),jnp.bfloat16),
        pltpu.VMEM((4,8,1024),jnp.int32), pltpu.SemaphoreType.DMA((12,))]


def partial_sums(valence, conduction, gvectors):
    z_tab, y_tab, x_tab = tables()
    return pl.pallas_call(
        transform_body,
        out_shape=jax.ShapeDtypeStruct((4, 2, 32, 1024), jnp.bfloat16),
        in_specs=[pl.BlockSpec(memory_space=pl.ANY)] * 6,
        out_specs=pl.BlockSpec(memory_space=pltpu.VMEM),
        scratch_shapes=transform_scratch(),
        compiler_params=pltpu.CompilerParams(vmem_limit_bytes=60 * 2**20),
        name="transform",
    )(valence.transpose(1, 0, 2), conduction.transpose(1, 0, 2), gvectors,
      jnp.asarray(z_tab), jnp.asarray(y_tab), jnp.asarray(x_tab, jnp.bfloat16))

MESH_AXES = ("y", "x", "zl", "core", "zh")
SIDE = pl.DeviceIdType.MESH
SUB = 256
WIDE = 4 * SUB


def turned(axis, step):
    size = lax.axis_size(axis)
    return lax.rem(lax.axis_index(axis) + step % size, size)


def remote(src, dst, send_sem, recv_sem, target):
    return pltpu.make_async_remote_copy(src_ref=src, dst_ref=dst, send_sem=send_sem, recv_sem=recv_sem,
                                        device_id=target, device_id_type=SIDE)


def pair_factor(val_energy, cond_energy, occupation):
    first = ((lax.axis_index("y") * 4 + lax.axis_index("x")) * 3 + lax.axis_index("zh")) * 2
    row = lax.broadcasted_iota(jnp.int32, (32, 16), 0)
    at_v = lax.broadcasted_iota(jnp.int32, (32, 16), 1) == (row & 15)
    ev = jnp.sum(jnp.where(at_v, val_energy, 0.0), axis=1, keepdims=True)
    occ = jnp.sum(jnp.where(at_v, occupation.astype(jnp.float32), 0.0), axis=1, keepdims=True)
    row = lax.broadcasted_iota(jnp.int32, (32, 192), 0)
    at_c = lax.broadcasted_iota(jnp.int32, (32, 192), 1) == first + (row >> 4)
    ec = jnp.sum(jnp.where(at_c, cond_energy, 0.0), axis=1, keepdims=True)
    return jnp.sqrt(occ / (4.0 * (ec - ev))) * (1.0 / N**1.5)


def exchange_body(parts, val_energy, cond_energy, occupation, out,
                  core_in, z_out, z_in, cols, rows, blocks, x_out, x_in,
                  core_sems, z_sems, zh_sems, y_sems, row_sems, row_out_sems, x_sems):
    y, x, zl, core, zh = (lax.axis_index(a) for a in MESH_AXES)
    barrier = pltpu.get_barrier_semaphore()
    partners = ([{"core": 1 - core}] + [{"zl": turned("zl", k)} for k in (1, 2, 3)]
                + [{"zh": turned("zh", k)} for k in (1, 2)] + [{"y": turned("y", k)} for k in (1, 7)]
                + [{"x": turned("x", k)} for k in (1, 2, 3)])
    for target in partners:
        pl.semaphore_signal(barrier, inc=1, device_id=target, device_id_type=SIDE)
    pl.semaphore_wait(barrier, len(partners))

    other = {"core": 1 - core}
    swaps = []
    for k in (2, 1, 3, 0):
        z = turned("zl", k)
        swaps.append((k, z, remote(parts.at[z, 1 - core], core_in.at[k], core_sems.at[0, k], core_sems.at[1, k], other)))
    for _, _, c in swaps:
        c.start()
    z_copies = []
    for k, z, c in swaps:
        c.wait_recv()
        both = parts[z, core].astype(jnp.float32) + core_in[k].astype(jnp.float32)
        if k:
            z_out[k - 1] = both.astype(jnp.bfloat16)
            c2 = remote(z_out.at[k - 1], z_in.at[k - 1], z_sems.at[0, k - 1], z_sems.at[1, k - 1], {"zl": z})
            c2.start()
            z_copies.append(c2)
        else:
            total = both
    factor = pair_factor(val_energy[...], cond_energy[...], occupation[...])
    for c in z_copies:
        c.wait_recv()
    for k in range(3):
        total = total + z_in[k].astype(jnp.float32)
    mine = zh * 8 + y
    cols[mine] = (total * factor).astype(jnp.bfloat16)

    zh_copies = []
    for k in (1, 2):
        c = remote(cols.at[mine], cols.at[mine], zh_sems.at[0, k - 1], zh_sems.at[1, k - 1], {"zh": turned("zh", k)})
        c.start()
        zh_copies.append(c)

    plane = 2 * zl + core
    home = y // 2
    on_chain = core == lax.rem(y, 2)
    source = plane == y

    def slot(t, step):
        return turned("zh", -t) * 8 + turned("y", step)

    def row_copy(n, s, i, target):
        return remote(rows.at[s], rows.at[s], row_out_sems.at[n, i], row_sems.at[n], target)

    def give_rows(t, step):
        n = t * 8 + step % 8
        s = slot(t, step)

        @pl.when(source)
        def _():
            for third in range(3):

                @pl.when(zh == third)
                def _():
                    for q in range(4):
                        rows[s, :, 80 * q : 80 * q + 80] = cols[s, :, SUB * q + 80 * third : SUB * q + 80 * third + 80]

            for k in (3, 2, 1):
                row_copy(n, s, k - 1, {"zl": turned("zl", k)}).start()
            row_copy(n, s, 3, other).start()

    def relay_rows(t, step):
        n = t * 8 + step % 8
        s = slot(t, step)

        @pl.when(on_chain & (zl != home))
        def _():
            row_copy(n, s, 3, other).wait_recv()
            row_copy(n, s, 3, other).start()

    def row_waits(act):
        for t in range(3):
            for step in range(8):
                act(t * 8 + step, slot(t, step))

    def ring(t, way, hop):
        s = slot(t, -way * (hop - 1))
        d = 0 if way == 1 else 1
        n = (t * 4 + hop - 1) * 2 + d
        half = pl.ds(0, 32) if hop < 4 else pl.ds(16 * d, 16)
        return remote(cols.at[s, half], cols.at[s, half], y_sems.at[0, n], y_sems.at[1, n], {"y": turned("y", way)})

    def landed(t, way, hop):
        s = slot(t, -way * hop)
        d = 0 if way == 1 else 1
        n = (t * 4 + hop - 1) * 2 + d
        half = pl.ds(0, 32) if hop < 4 else pl.ds(16 * d, 16)
        remote(cols.at[s, half], cols.at[s, half], y_sems.at[0, n], y_sems.at[1, n], {"y": turned("y", way)}).wait_recv()

    def start(t, hop):
        ring(t, 1, hop).start()
        ring(t, -1, hop).start()

    start(0, 1)
    give_rows(0, 0)
    for hop in (1, 2, 3):
        landed(0, 1, hop)
        ring(0, 1, hop + 1).start()
        landed(0, -1, hop)
        ring(0, -1, hop + 1).start()
        give_rows(0, -hop)
        give_rows(0, hop)
        if hop == 2:
            for t in (1, 2):
                zh_copies[t - 1].wait_recv()
                start(t, 1)
            for t in (1, 2):
                give_rows(t, 0)
    for step in (0, 1, -1, 2, -2):
        relay_rows(0, step)
    landed(0, 1, 4)
    landed(0, -1, 4)
    give_rows(0, 4)
    for t in (1, 2):
        relay_rows(t, 0)
    for hop in (1, 2, 3):
        for t in (1, 2):
            landed(t, 1, hop)
            ring(t, 1, hop + 1).start()
            landed(t, -1, hop)
            ring(t, -1, hop + 1).start()
        for t in (1, 2):
            give_rows(t, -hop)
            give_rows(t, hop)
        if hop == 1:
            for step in (3, -3, 4):
                relay_rows(0, step)
        else:
            for t in (1, 2):
                relay_rows(t, hop - 1)
                relay_rows(t, 1 - hop)
    for t in (1, 2):
        landed(t, 1, 4)
        landed(t, -1, 4)
        give_rows(t, 4)
    for t in (1, 2):
        for step in (3, -3, 4):
            relay_rows(t, step)

    @pl.when(jnp.logical_not(on_chain))
    def _():
        row_waits(lambda n, s: row_copy(n, s, 3, other).wait_recv())

    left = rows[:, :, 0:320].reshape(768, 320)
    right = cols[...].reshape(768, WIDE)
    blocks[...] = lax.dot_general(left, right, (((0,), (0,)), ((), ())), preferred_element_type=jnp.float32)
    x_copies = []
    for k in (2, 1, 3):
        q = turned("x", k)
        x_out[k - 1] = blocks[pl.ds(pl.multiple_of(80 * q, 80), 80)].astype(jnp.bfloat16)
        c = remote(x_out.at[k - 1], x_in.at[k - 1], x_sems.at[0, k - 1], x_sems.at[1, k - 1], {"x": q})
        c.start()
        x_copies.append(c)
    total = blocks[pl.ds(pl.multiple_of(80 * x, 80), 80)]
    for c in x_copies:
        c.wait_recv()
    for k in range(3):
        total = total + x_in[k].astype(jnp.float32)
    out[...] = total * (-1.0 / math.sqrt(3072))

    for _, _, c in swaps:
        c.wait_send()
    for c in z_copies + zh_copies + x_copies:
        c.wait_send()
    for t in range(3):
        for hop in (1, 2, 3, 4):
            ring(t, 1, hop).wait_send()
            ring(t, -1, hop).wait_send()

    @pl.when(source)
    def _():
        for i in range(4):
            row_waits(lambda n, s: row_copy(n, s, i, other).wait_send())

    @pl.when(on_chain & (zl != home))
    def _():
        row_waits(lambda n, s: row_copy(n, s, 3, other).wait_send())


def exchange_scratch():
    dma = pltpu.SemaphoreType.DMA
    return [
        pltpu.VMEM((4, 32, WIDE), jnp.bfloat16),
        pltpu.VMEM((3, 32, WIDE), jnp.bfloat16),
        pltpu.VMEM((3, 32, WIDE), jnp.bfloat16),
        pltpu.VMEM((24, 32, WIDE), jnp.bfloat16),
        pltpu.VMEM((24, 32, 384), jnp.bfloat16),
        pltpu.VMEM((320, WIDE), jnp.float32),
        pltpu.VMEM((3, 80, WIDE), jnp.bfloat16),
        pltpu.VMEM((3, 80, WIDE), jnp.bfloat16),
        dma((2, 4)), dma((2, 3)), dma((2, 2)), dma((2, 24)), dma((24,)), dma((24, 4)), dma((2, 3)),
    ]


def exchange(parts, val_energy, cond_energy, occupation):
    return pl.pallas_call(
        exchange_body,
        out_shape=jax.ShapeDtypeStruct((80, WIDE), jnp.float32),
        in_specs=[pl.BlockSpec(memory_space=pltpu.VMEM)] * 4,
        out_specs=pl.BlockSpec(memory_space=pltpu.VMEM),
        scratch_shapes=exchange_scratch(),
        compiler_params=pltpu.CompilerParams(collective_id=0, has_side_effects=True, vmem_limit_bytes=60 * 2**20),
        name="exchange",
    )(parts, val_energy, cond_energy, occupation)


def body(valence, conduction, val_energy, cond_energy, val_occupation, gvectors):
    parts = partial_sums(valence, conduction, gvectors)
    chi = exchange(parts, val_energy.reshape(1, 16), cond_energy.reshape(1, 192), val_occupation.reshape(1, 16))
    return jnp.concatenate([chi[:, SUB * q : SUB * q + 240] for q in range(4)], axis=1)


def solution(mesh):
    finer = Mesh(mesh.devices.reshape(8, 4, 4, 2, 3), MESH_AXES)
    grow = ("zl", "core")
    bands = ("y", "x", "zh")
    placed = (P(None, grow, None), P(bands, grow, None), P(), P(), P(), P())
    return jax.shard_map(body, mesh=finer, in_specs=placed, out_specs=P(bands, grow), check_vma=False)
```

```python
import functools
import math

import jax
import jax.numpy as jnp
import numpy as np
from jax import lax
from jax.experimental import pallas as pl
from jax.experimental.pallas import tpu as pltpu
from jax.sharding import Mesh
from jax.sharding import PartitionSpec as P

N=96; RAD=12; KG=3840; NV=16
PL=12
PART=1152
HALF=math.sqrt(0.5)

def lane_waves():
    j=np.zeros((4,128),np.int64); k=np.zeros((4,128),np.int64); used=np.zeros((4,2,128))
    for l in range(91):
        j[0,l],k[0,l]=(-8+8*(l//13),l%13) if l<39 else (-12+8*((l-39)//13),(l-39)%13)
        used[0,0 if l<39 else 1,l]=1
    for c in (1,2,3):
        for l in range(75):
            j[c,l],k[c,l]=c-8+8*(l//25),l%25-12
            used[c,:,l]=1
    return j,k,used

def phase_of(n): return 2*np.pi*np.mod(n,N)/N

def tables():
    j,k,used=lane_waves()
    z=np.arange(N); y=np.arange(12)
    kz=phase_of(z[None,:,None]*k[:2,None,:])
    z_tab=np.stack([np.cos(kz),np.sin(kz)],1).astype(np.float32)
    jy=phase_of(y[None,:,None]*j[:,None,:])
    y_tab=np.stack([np.cos(jy),np.sin(jy)],1)
    first=np.where(used[:,0,None,None,:]>0,y_tab,0.0)
    y_tab0=np.where(used[0,1,None,None,:]>0,y_tab[0],0.0)
    y_all=np.concatenate([first,y_tab0[None]],0).astype(np.float32)
    a=np.arange(16)
    X=np.arange(N).reshape(8,12)
    ax=phase_of(X[:,:,None]*a[None,None,:])
    x_tab=np.zeros((8,32,16),np.float32)
    x_tab[:,:12]=np.cos(ax); x_tab[:,16:28]=np.sin(ax)
    return z_tab,y_all,x_tab

def sections(val, con, gvec_in, z_in, y_in, x_in, vbuf, cbuf, gvec, z_tab, y_tab, x_tab, tab, mixed, sec_re, sec_im, keys, sems):
    grow=2*lax.axis_index("zl")+lax.axis_index("core")
    small=[pltpu.make_async_copy(a,b,sems.at[8+i]) for i,(a,b) in enumerate([(z_in,z_tab),(y_in,y_tab),(gvec_in,gvec),(x_in.at[grow],x_tab)])]
    for c in small: c.start()
    copies=[]
    for s in range(4):
        copies.append((pltpu.make_async_copy(val.at[pl.ds(3*s,3)],vbuf.at[pl.ds(3*s,3)],sems.at[s]),
                       pltpu.make_async_copy(con.at[pl.ds(3*s,3)],cbuf.at[pl.ds(3*s,3)],sems.at[4+s])))
    for pair in copies:
        for c in pair: c.start()
    for c in small: c.wait()
    with jax.named_scope("tables"):
        def build(yp,_):
            row=pl.ds(pl.multiple_of(yp*N,32),N)
            for t in range(4):
                cz=z_tab[min(t,1),0]; sz=z_tab[min(t,1),1]
                cy=y_tab[t,0,pl.ds(yp,1)]; sy=y_tab[t,1,pl.ds(yp,1)]
                co=(cy*cz-sy*sz); si=(sy*cz+cy*sz)
                tab[t,row,0:128]=co.astype(jnp.bfloat16)
                tab[t,row,128:256]=si.astype(jnp.bfloat16)
                row2=pl.ds(pl.multiple_of(PART+yp*N,32),N)
                if t==0:
                    cy=y_tab[4,0,pl.ds(yp,1)]; sy=y_tab[4,1,pl.ds(yp,1)]
                    tab[t,row2,0:128]=(cy*cz-sy*sz).astype(jnp.bfloat16)
                    tab[t,row2,128:256]=(sy*cz+cy*sz).astype(jnp.bfloat16)
                else:
                    tab[t,row2,0:128]=(-si).astype(jnp.bfloat16)
                    tab[t,row2,128:256]=co.astype(jnp.bfloat16)
            return 0
        lax.fori_loop(0,12,build,0)
    keys[...] = jnp.zeros_like(keys)
    for b in range(16):
        lanes=pl.ds(240*b,240)
        a=gvec[0:1,lanes]; j=gvec[1:2,lanes]; k=gvec[2:3,lanes]
        j8=j&7
        flip=(j8>=5)|(((j8&3)==0)&((k<0)|((k==0)&(j<0))))
        j=jnp.where(flip,-j,j); k=jnp.where(flip,-k,k)
        c=j&7
        odd=128*c+25*((j+8-c)>>3)+k+12
        even=jnp.where(c==0,13*((j+8)>>3)+k,39+13*((j+12)>>3)+k)
        lanes=pl.ds(256*(b%4),240)
        keys[b//4,0:1,lanes]=jnp.where((c&3)==0,even,odd)
        keys[b//4,1:2,lanes]=a
        keys[b//4,2:3,lanes]=flip.astype(jnp.int32)
    with jax.named_scope("mix"):
        def mix(x,_):
            for c in range(2):
                row=pl.ds(pl.multiple_of(x*32+16*c,16),16)
                for w in range(0,PART,384):
                    d=[]
                    for q in range(8):
                        lanes=pl.ds(q*PART+w,384)
                        d.append((vbuf[x,:,lanes]*cbuf[x,c:c+1,lanes]).astype(jnp.float32))
                    a=[d[q]+d[q+4] for q in range(4)]
                    m=[d[q]-d[q+4] for q in range(4)]
                    p=(m[1]-m[3])*HALF; r=(m[1]+m[3])*HALF
                    even=a[0]+a[2]; odd=a[1]+a[3]
                    for t,(u,v) in enumerate([(even+odd,even-odd),(m[0]+p,m[2]+r),(a[0]-a[2],a[1]-a[3]),(m[0]-p,r-m[2])]):
                        mixed[t,row,w:w+384]=u.astype(jnp.bfloat16)
                        mixed[t,row,PART+w:PART+w+384]=v.astype(jnp.bfloat16)
            return 0
        for s in range(4):
            for c in copies[s]: c.wait()
            lax.fori_loop(3*s,3*s+3,mix,0)
    with jax.named_scope("planes"):
        for t in range(4):
            both=jnp.dot(mixed[t],tab[t],preferred_element_type=jnp.float32)
            sec_re[:,128*t:128*(t+1)]=both[:,:128].astype(jnp.bfloat16)
            sec_im[:,128*t:128*(t+1)]=both[:,128:].astype(jnp.bfloat16)

def pick(b, out, x_tab, sec_re, sec_im, keys):
    waves=x_tab[...]
    for n0 in range(0,1024,256):
        w=256
        lanes=pl.ds(n0,w)
        rho=keys[b,0:1,lanes]; a=keys[b,1:2,lanes]; sign=1.0-2.0*keys[b,2:3,lanes].astype(jnp.float32)
        hot=(lax.broadcasted_iota(jnp.int32,(512,w),0)==rho).astype(jnp.float32).astype(jnp.bfloat16)
        hot_a=(lax.broadcasted_iota(jnp.int32,(16,w),0)==a).astype(jnp.float32).astype(jnp.bfloat16)
        wave=jnp.dot(waves,hot_a,preferred_element_type=jnp.float32)
        re=jnp.dot(sec_re[...],hot,preferred_element_type=jnp.float32)
        im=jnp.dot(sec_im[...],hot,preferred_element_type=jnp.float32)
        tot_re=jnp.zeros((32,w),jnp.float32); tot_im=jnp.zeros((32,w),jnp.float32)
        for x in range(PL):
            co=wave[x:x+1]; si=wave[16+x:17+x]
            gr=re[32*x:32*x+32]; gi=im[32*x:32*x+32]
            tot_re+=co*gr-(si*sign)*gi
            tot_im+=si*gr+(co*sign)*gi
        out[b//2,lax.rem(b,2),:,lanes]=tot_re.astype(out.dtype)
        out[2+b//2,lax.rem(b,2),:,lanes]=(-tot_im).astype(out.dtype)


MESH_AXES = ("y", "x", "zl", "core", "zh")
SIDE = pl.DeviceIdType.MESH
SUB = 256
WIDE = 4 * SUB


def turned(axis, step):
    size = lax.axis_size(axis)
    return lax.rem(lax.axis_index(axis) + step % size, size)


def remote(src, dst, send_sem, recv_sem, target):
    return pltpu.make_async_remote_copy(src_ref=src, dst_ref=dst, send_sem=send_sem, recv_sem=recv_sem,
                                        device_id=target, device_id_type=SIDE)


def pair_factor(val_energy, cond_energy, occupation):
    first = ((lax.axis_index("y") * 4 + lax.axis_index("x")) * 3 + lax.axis_index("zh")) * 2
    row = lax.broadcasted_iota(jnp.int32, (32, 16), 0)
    at_v = lax.broadcasted_iota(jnp.int32, (32, 16), 1) == (row & 15)
    ev = jnp.sum(jnp.where(at_v, val_energy, 0.0), axis=1, keepdims=True)
    occ = jnp.sum(jnp.where(at_v, occupation.astype(jnp.float32), 0.0), axis=1, keepdims=True)
    row = lax.broadcasted_iota(jnp.int32, (32, 192), 0)
    at_c = lax.broadcasted_iota(jnp.int32, (32, 192), 1) == first + (row >> 4)
    ec = jnp.sum(jnp.where(at_c, cond_energy, 0.0), axis=1, keepdims=True)
    return jnp.sqrt(occ / (4.0 * (ec - ev))) * (1.0 / N**1.5)


def fused_body(val, con, gvec_in, z_tab_in, y_tab_in, x_tab_in, val_energy, cond_energy, occupation, out,
                  vbuf, cbuf, gvec, z_tab, y_tab, x_tab, tab, mixed, sec_re, sec_im, keys, load_sems, parts,
                  core_in, z_out, z_in, cols, rows, blocks, x_out, x_in,
                  core_sems, z_sems, zh_sems, y_sems, row_sems, row_out_sems, x_sems):
    y, x, zl, core, zh = (lax.axis_index(a) for a in MESH_AXES)
    barrier = pltpu.get_barrier_semaphore()
    partners = ([{"core": 1 - core}] + [{"zl": turned("zl", k)} for k in (1, 2, 3)]
                + [{"zh": turned("zh", k)} for k in (1, 2)] + [{"y": turned("y", k)} for k in (1, 7)]
                + [{"x": turned("x", k)} for k in (1, 2, 3)])
    for target in partners:
        pl.semaphore_signal(barrier, inc=1, device_id=target, device_id_type=SIDE)

    sections(val, con, gvec_in, z_tab_in, y_tab_in, x_tab_in, vbuf, cbuf, gvec, z_tab, y_tab, x_tab, tab, mixed,
             sec_re, sec_im, keys, load_sems)
    with jax.named_scope("barrier"):
        pl.semaphore_wait(barrier, len(partners))

    other = {"core": 1 - core}
    odd = 1 - lax.rem(zl, 2)

    def swap(k):
        return remote(parts.at[turned("zl", k), 1 - core], core_in.at[k], core_sems.at[0, k], core_sems.at[1, k], other)

    def pass_on(k):
        return remote(z_out.at[k - 1], z_in.at[k - 1], z_sems.at[0, k - 1], z_sems.at[1, k - 1], {"zl": turned("zl", k)})

    def both_cores(k):
        swap(k).wait_recv()
        return parts[turned("zl", k), core].astype(jnp.float32) + core_in[k].astype(jnp.float32)

    with jax.named_scope("picks"):
        pick(2 * odd + 1 - core, parts, x_tab, sec_re, sec_im, keys)
        for k in (1, 3):
            swap(k).start()
        pick(2 * (1 - odd) + 1 - core, parts, x_tab, sec_re, sec_im, keys)
        for k in (2, 0):
            swap(k).start()
        pick(2 * odd + core, parts, x_tab, sec_re, sec_im, keys)
        for k in (1, 3):
            z_out[k - 1] = both_cores(k).astype(jnp.bfloat16)
            pass_on(k).start()
        pick(2 * (1 - odd) + core, parts, x_tab, sec_re, sec_im, keys)
        z_out[1] = both_cores(2).astype(jnp.bfloat16)
        pass_on(2).start()
        total = both_cores(0)
    factor = pair_factor(val_energy[...], cond_energy[...], occupation[...])
    with jax.named_scope("zsum"):
        for k in (1, 3, 2):
            pass_on(k).wait_recv()
            total = total + z_in[k - 1].astype(jnp.float32)
    mine = zh * 8 + y
    cols[mine] = (total * factor).astype(jnp.bfloat16)

    zh_copies = []
    for k in (1, 2):
        c = remote(cols.at[mine], cols.at[mine], zh_sems.at[0, k - 1], zh_sems.at[1, k - 1], {"zh": turned("zh", k)})
        c.start()
        zh_copies.append(c)

    plane = 2 * zl + core
    home = y // 2
    on_chain = core == lax.rem(y, 2)
    source = plane == y

    def slot(t, step):
        return turned("zh", -t) * 8 + turned("y", step)

    def row_copy(n, s, i, target):
        return remote(rows.at[s], rows.at[s], row_out_sems.at[n, i], row_sems.at[n], target)

    def give_rows(t, step):
        n = t * 8 + step % 8
        s = slot(t, step)

        @pl.when(source)
        def _():
            for third in range(3):

                @pl.when(zh == third)
                def _():
                    for q in range(4):
                        rows[s, :, 80 * q : 80 * q + 80] = cols[s, :, SUB * q + 80 * third : SUB * q + 80 * third + 80]

            for k in (3, 2, 1):
                row_copy(n, s, k - 1, {"zl": turned("zl", k)}).start()
            row_copy(n, s, 3, other).start()

    def relay_rows(t, step):
        n = t * 8 + step % 8
        s = slot(t, step)

        @pl.when(on_chain & (zl != home))
        def _():
            row_copy(n, s, 3, other).wait_recv()
            row_copy(n, s, 3, other).start()

    def row_waits(act):
        for t in range(3):
            for step in range(8):
                act(t * 8 + step, slot(t, step))

    def ring(t, way, hop):
        s = slot(t, -way * (hop - 1))
        d = 0 if way == 1 else 1
        n = (t * 4 + hop - 1) * 2 + d
        half = pl.ds(0, 32) if hop < 4 else pl.ds(16 * d, 16)
        return remote(cols.at[s, half], cols.at[s, half], y_sems.at[0, n], y_sems.at[1, n], {"y": turned("y", way)})

    def landed(t, way, hop):
        s = slot(t, -way * hop)
        d = 0 if way == 1 else 1
        n = (t * 4 + hop - 1) * 2 + d
        half = pl.ds(0, 32) if hop < 4 else pl.ds(16 * d, 16)
        remote(cols.at[s, half], cols.at[s, half], y_sems.at[0, n], y_sems.at[1, n], {"y": turned("y", way)}).wait_recv()

    def start(t, hop):
        ring(t, 1, hop).start()
        ring(t, -1, hop).start()

    with jax.named_scope("ring0"):
        start(0, 1)
        give_rows(0, 0)
        for hop in (1, 2, 3):
            landed(0, 1, hop)
            ring(0, 1, hop + 1).start()
            landed(0, -1, hop)
            ring(0, -1, hop + 1).start()
            give_rows(0, -hop)
            give_rows(0, hop)
            if hop == 2:
                for t in (1, 2):
                    with jax.named_scope("zh"):
                        zh_copies[t - 1].wait_recv()
                    start(t, 1)
                for t in (1, 2):
                    give_rows(t, 0)
    with jax.named_scope("relay0"):
        for step in (0, 1, -1, 2, -2):
            relay_rows(0, step)
    with jax.named_scope("ring04"):
        landed(0, 1, 4)
        landed(0, -1, 4)
        give_rows(0, 4)
        for t in (1, 2):
            relay_rows(t, 0)
    for hop in (1, 2, 3):
        for t in (1, 2):
            with jax.named_scope("ring%d%d" % (t, hop)):
                landed(t, 1, hop)
                ring(t, 1, hop + 1).start()
                landed(t, -1, hop)
                ring(t, -1, hop + 1).start()
        for t in (1, 2):
            give_rows(t, -hop)
            give_rows(t, hop)
        if hop == 1:
            for step in (3, -3, 4):
                relay_rows(0, step)
        else:
            for t in (1, 2):
                relay_rows(t, hop - 1)
                relay_rows(t, 1 - hop)
    with jax.named_scope("ring124"):
        for t in (1, 2):
            landed(t, 1, 4)
            landed(t, -1, 4)
            give_rows(t, 4)
    with jax.named_scope("rowwait"):
        for t in (1, 2):
            for step in (3, -3, 4):
                relay_rows(t, step)

        @pl.when(jnp.logical_not(on_chain))
        def _():
            row_waits(lambda n, s: row_copy(n, s, 3, other).wait_recv())

    with jax.named_scope("matmul"):
        left = rows[:, :, 0:320].reshape(768, 320)
        right = cols[...].reshape(768, WIDE)
        blocks[...] = lax.dot_general(left, right, (((0,), (0,)), ((), ())), preferred_element_type=jnp.float32)
        x_copies = []
        for k in (2, 1, 3):
            q = turned("x", k)
            x_out[k - 1] = blocks[pl.ds(pl.multiple_of(80 * q, 80), 80)].astype(jnp.bfloat16)
            c = remote(x_out.at[k - 1], x_in.at[k - 1], x_sems.at[0, k - 1], x_sems.at[1, k - 1], {"x": q})
            c.start()
            x_copies.append(c)
        total = blocks[pl.ds(pl.multiple_of(80 * x, 80), 80)]
    with jax.named_scope("xsum"):
        for c in x_copies:
            c.wait_recv()
        for k in range(3):
            total = total + x_in[k].astype(jnp.float32)
    total = total * (-1.0 / math.sqrt(3072))
    for q in range(4):
        out[:, 240 * q : 240 * q + 240] = total[:, SUB * q : SUB * q + 240]

    for k in range(4):
        swap(k).wait_send()
    for k in (1, 2, 3):
        pass_on(k).wait_send()
    for c in zh_copies + x_copies:
        c.wait_send()
    for t in range(3):
        for hop in (1, 2, 3, 4):
            ring(t, 1, hop).wait_send()
            ring(t, -1, hop).wait_send()

    @pl.when(source)
    def _():
        for i in range(4):
            row_waits(lambda n, s: row_copy(n, s, i, other).wait_send())

    @pl.when(on_chain & (zl != home))
    def _():
        row_waits(lambda n, s: row_copy(n, s, 3, other).wait_send())


def fused_scratch():
    dma = pltpu.SemaphoreType.DMA
    return [
        pltpu.VMEM((PL, NV, 9216), jnp.bfloat16),
        pltpu.VMEM((PL, 2, 9216), jnp.bfloat16),
        pltpu.VMEM((3, KG), jnp.int32),
        pltpu.VMEM((2, 2, 96, 128), jnp.float32),
        pltpu.VMEM((5, 2, 12, 128), jnp.float32),
        pltpu.VMEM((32, 16), jnp.bfloat16),
        pltpu.VMEM((4, 2 * PART, 256), jnp.bfloat16),
        pltpu.VMEM((4, 384, 2 * PART), jnp.bfloat16),
        pltpu.VMEM((384, 512), jnp.bfloat16),
        pltpu.VMEM((384, 512), jnp.bfloat16),
        pltpu.VMEM((4, 8, 1024), jnp.int32),
        dma((12,)),
        pltpu.VMEM((4, 2, 32, WIDE), jnp.bfloat16),
        pltpu.VMEM((4, 32, WIDE), jnp.bfloat16),
        pltpu.VMEM((3, 32, WIDE), jnp.bfloat16),
        pltpu.VMEM((3, 32, WIDE), jnp.bfloat16),
        pltpu.VMEM((24, 32, WIDE), jnp.bfloat16),
        pltpu.VMEM((24, 32, 384), jnp.bfloat16),
        pltpu.VMEM((320, WIDE), jnp.float32),
        pltpu.VMEM((3, 80, WIDE), jnp.bfloat16),
        pltpu.VMEM((3, 80, WIDE), jnp.bfloat16),
        dma((2, 4)), dma((2, 3)), dma((2, 2)), dma((2, 24)), dma((24,)), dma((24, 4)), dma((2, 3)),
    ]


def body(valence, conduction, val_energy, cond_energy, val_occupation, gvectors):
    z_tab, y_tab, x_tab = tables()
    return pl.pallas_call(
        fused_body,
        out_shape=jax.ShapeDtypeStruct((80, 960), jnp.float32),
        in_specs=[pl.BlockSpec(memory_space=pl.ANY)] * 6 + [pl.BlockSpec(memory_space=pltpu.VMEM)] * 3,
        out_specs=pl.BlockSpec(memory_space=pltpu.VMEM),
        scratch_shapes=fused_scratch(),
        compiler_params=pltpu.CompilerParams(collective_id=0, has_side_effects=True, vmem_limit_bytes=60 * 2**20),
        name="chi",
    )(valence.transpose(1, 0, 2), conduction.transpose(1, 0, 2), gvectors,
      jnp.asarray(z_tab), jnp.asarray(y_tab), jnp.asarray(x_tab, jnp.bfloat16),
      val_energy.reshape(1, 16), cond_energy.reshape(1, 192), val_occupation.reshape(1, 16))


def solution(mesh):
    finer = Mesh(mesh.devices.reshape(8, 4, 4, 2, 3), MESH_AXES)
    grow = ("zl", "core")
    bands = ("y", "x", "zh")
    placed = (P(None, grow, None), P(bands, grow, None), P(), P(), P(), P())
    return jax.shard_map(body, mesh=finer, in_specs=placed, out_specs=P(bands, grow), check_vma=False)
```

```python
import heapq
import math

import jax
import jax.numpy as jnp
import numpy as np
from jax import lax
from jax.experimental import pallas as pl
from jax.experimental.pallas import tpu as pltpu
from jax.sharding import Mesh
from jax.sharding import PartitionSpec as P

N = 96
RAD = 12
KG = 3840
NV = 16
PLANES = 12
PART = 1152
QUARTER = 240
SUB = 256
MESH_AXES = ("y", "x", "zl", "core", "zh")
SIDE = pl.DeviceIdType.MESH
scope = jax.named_scope


def phase_of(n):
    return 2 * np.pi * np.mod(n, N) / N


def tables():
    j = np.zeros((4, 128), np.int64)
    k = np.zeros((4, 128), np.int64)
    used = np.zeros((4, 2, 128))
    for l in range(91):
        j[0, l], k[0, l] = (-8 + 8 * (l // 13), l % 13) if l < 39 else (-12 + 8 * ((l - 39) // 13), (l - 39) % 13)
        used[0, 0 if l < 39 else 1, l] = 1
    for c in (1, 2, 3):
        for l in range(75):
            j[c, l], k[c, l] = c - 8 + 8 * (l // 25), l % 25 - 12
            used[c, :, l] = 1
    kz = phase_of(np.arange(N)[None, :, None] * k[:2, None, :])
    z_tab = np.stack([np.cos(kz), np.sin(kz)], 1).astype(np.float32)
    jy = phase_of(np.arange(12)[None, :, None] * j[:, None, :])
    waves = np.stack([np.cos(jy), np.sin(jy)], 1)
    first = np.where(used[:, 0, None, None, :] > 0, waves, 0.0)
    second = np.where(used[0, 1, None, None, :] > 0, waves[0], 0.0)
    y_tab = np.concatenate([first, second[None]], 0).astype(np.float32)
    ax = phase_of(np.arange(N).reshape(8, 12)[:, :, None] * np.arange(16)[None, None, :])
    x_tab = np.zeros((8, 32, 16), np.float32)
    x_tab[:, :12] = np.cos(ax)
    x_tab[:, 16:28] = np.sin(ax)
    return z_tab, y_tab, x_tab


def build_waves(t, z_tab, y_tab, tab):
    cz = z_tab[min(t, 1), 0]
    sz = z_tab[min(t, 1), 1]
    for y in range(12):
        row = slice(y * N, (y + 1) * N)
        below = slice(PART + y * N, PART + (y + 1) * N)
        cy = y_tab[t, 0, y : y + 1]
        sy = y_tab[t, 1, y : y + 1]
        co = (cy * cz - sy * sz).astype(jnp.bfloat16)
        si = (sy * cz + cy * sz).astype(jnp.bfloat16)
        tab[t, row, 0:128] = co
        tab[t, row, 128:256] = si
        if t == 0:
            cy = y_tab[4, 0, y : y + 1]
            sy = y_tab[4, 1, y : y + 1]
            tab[t, below, 0:128] = (cy * cz - sy * sz).astype(jnp.bfloat16)
            tab[t, below, 128:256] = (sy * cz + cy * sz).astype(jnp.bfloat16)
        else:
            tab[t, below, 0:128] = -si
            tab[t, below, 128:256] = co


def build_keys(gvec, keys):
    keys[...] = jnp.zeros_like(keys)
    for b in range(16):
        lanes = pl.ds(QUARTER * b, QUARTER)
        a = gvec[0:1, lanes]
        j = gvec[1:2, lanes]
        k = gvec[2:3, lanes]
        j8 = j & 7
        flip = (j8 >= 5) | (((j8 & 3) == 0) & ((k < 0) | ((k == 0) & (j < 0))))
        j = jnp.where(flip, -j, j)
        k = jnp.where(flip, -k, k)
        c = j & 7
        odd = 128 * c + 25 * ((j + 8 - c) >> 3) + k + 12
        even = jnp.where(c == 0, 13 * ((j + 8) >> 3) + k, 39 + 13 * ((j + 12) >> 3) + k)
        lanes = pl.ds(SUB * (b % 4), QUARTER)
        keys[b // 4, 0:1, lanes] = jnp.where((c & 3) == 0, even, odd)
        keys[b // 4, 1:2, lanes] = a
        keys[b // 4, 2:3, lanes] = flip.astype(jnp.int32)


def mix_planes(first, last, vbuf, cbuf, wide, mixed):
    half = jnp.asarray(math.sqrt(0.5), jnp.bfloat16)

    def mix(x, _):
        wide[x] = cbuf[x].astype(jnp.float32)
        for c in range(2):
            row = pl.ds(pl.multiple_of(x * 32 + 16 * c, 16), 16)
            for w in range(0, PART, 384):
                d = []
                for q in range(8):
                    lanes = pl.ds(q * PART + w, 384)
                    band = jnp.broadcast_to(wide[x, c : c + 1, lanes], (16, 384)).astype(jnp.bfloat16)
                    d.append(vbuf[x, :, lanes] * band)
                a = [d[q] + d[q + 4] for q in range(4)]
                m = [d[q] - d[q + 4] for q in range(4)]
                p = (m[1] - m[3]) * half
                r = (m[1] + m[3]) * half
                even = a[0] + a[2]
                odd = a[1] + a[3]
                sums = [(even + odd, even - odd), (m[0] + p, m[2] + r), (a[0] - a[2], a[1] - a[3]), (m[0] - p, r - m[2])]
                for t, (u, v) in enumerate(sums):
                    mixed[t, row, w : w + 384] = u
                    mixed[t, row, PART + w : PART + w + 384] = v
        return 0

    lax.fori_loop(first, last, mix, 0)


def plane_sums(t, mixed, tab, sec):
    both = jnp.dot(mixed[t], tab[t], preferred_element_type=jnp.float32)
    for part in range(2):
        values = both[:, 128 * part : 128 * (part + 1)].astype(jnp.bfloat16)
        sec[:, part, :, 128 * t : 128 * (t + 1)] = values.reshape(PLANES, 32, 128)


def pick(b, q, parts, x_tab, sec, keys):
    lanes = pl.ds(SUB * q, SUB)
    sign = 1.0 - 2.0 * keys[b, 2:3, lanes].astype(jnp.float32)
    hot = (lax.broadcasted_iota(jnp.int32, (512, SUB), 0) == keys[b, 0:1, lanes]).astype(jnp.float32).astype(jnp.bfloat16)
    hot_a = (lax.broadcasted_iota(jnp.int32, (16, SUB), 0) == keys[b, 1:2, lanes]).astype(jnp.float32).astype(jnp.bfloat16)
    wave = jnp.dot(x_tab[...], hot_a, preferred_element_type=jnp.float32)
    got = jnp.dot(sec[...].reshape(64 * PLANES, 512), hot, preferred_element_type=jnp.float32)
    re = jnp.zeros((32, SUB), jnp.float32)
    im = jnp.zeros((32, SUB), jnp.float32)
    for x in range(PLANES):
        co = wave[x : x + 1]
        si = wave[16 + x : 17 + x]
        g_re = got[64 * x : 64 * x + 32]
        g_im = got[64 * x + 32 : 64 * x + 64]
        re += co * g_re - (si * sign) * g_im
        im += si * g_re + (co * sign) * g_im
    parts[b // 2, lax.rem(b, 2), q] = re.astype(parts.dtype)
    parts[2 + b // 2, lax.rem(b, 2), q] = (-im).astype(parts.dtype)


def pair_factor(val_energy, cond_energy, occupation):
    first = ((lax.axis_index("y") * 4 + lax.axis_index("x")) * 3 + lax.axis_index("zh")) * 2
    row = lax.broadcasted_iota(jnp.int32, (32, 16), 0)
    at_v = lax.broadcasted_iota(jnp.int32, (32, 16), 1) == (row & 15)
    ev = jnp.sum(jnp.where(at_v, val_energy, 0.0), axis=1, keepdims=True)
    occ = jnp.sum(jnp.where(at_v, occupation.astype(jnp.float32), 0.0), axis=1, keepdims=True)
    row = lax.broadcasted_iota(jnp.int32, (32, 192), 0)
    at_c = lax.broadcasted_iota(jnp.int32, (32, 192), 1) == first + (row >> 4)
    ec = jnp.sum(jnp.where(at_c, cond_energy, 0.0), axis=1, keepdims=True)
    return jnp.sqrt(occ / (4.0 * (ec - ev))) * (1.0 / N**1.5)


EARLY = 8
CHAINED = 20


def step_of(way, hop):
    return 4 if hop == 4 else -way * hop


def carried(way, hop):
    return (0, 1) if hop < 4 else ((0,) if way == 1 else (1,))


RING = [(t, way, hop, h) for t in range(3) for way in (1, -1) for hop in (1, 2, 3, 4) for h in carried(way, hop)]
RING_AT = {piece: i for i, piece in enumerate(RING)}


def timetable(zh):
    ready = (0.0, 2.3, 4.6)
    queue = []
    for h in range(2):
        heapq.heappush(queue, (ready[zh] + 0.42 * h, 0, ("own", h)))
        for t in (1, 2):
            there = max(ready[(zh - t) % 3] + 6.84, ready[zh] + 1.87)
            heapq.heappush(queue, (there + 2.62 * h, 1, ("zh", t, h)))
    free = {1: 0.0, -1: 0.0}
    left = {(t, step): 2 for t in range(3) for step in range(-3, 5)}
    slot = {}
    order = []

    def send(now, t, way, hop, h):
        free[way] = max(free[way], now) + 0.96
        heapq.heappush(queue, (free[way] + 4.43, 2, ("ring", t, way, hop, h)))

    def have(now, t, step):
        left[t, step] -= 1
        if not left[t, step]:
            slot[t, step] = len(slot)
            heapq.heappush(queue, (now, 3, ("give", t, step)))
            for far in (1, 2, 3) if slot[t, step] < CHAINED else (1,):
                heapq.heappush(queue, (now + 3.67 + 3.14 * far, 4, ("relay", t, step, far)))

    while queue:
        now, _, event = heapq.heappop(queue)
        order.append(event)
        if event[0] in ("own", "zh"):
            t, h = (0, event[1]) if event[0] == "own" else event[1:]
            for way in (1, -1):
                send(now, t, way, 1, h)
            have(now, t, 0)
        elif event[0] == "ring":
            _, t, way, hop, h = event
            if hop < 4 and h in carried(way, hop + 1):
                send(now, t, way, hop + 1, h)
            have(now, t, step_of(way, hop))
    return order, slot


TABLES = [timetable(zh) for zh in range(3)]


def turned(axis, step):
    size = lax.axis_size(axis)
    return lax.rem(lax.axis_index(axis) + step % size, size)


def remote(src, dst, send_sem, recv_sem, target):
    return pltpu.make_async_remote_copy(
        src_ref=src, dst_ref=dst, send_sem=send_sem, recv_sem=recv_sem, device_id=target, device_id_type=SIDE
    )


def chi_body(
    val, con, gvec_in, z_in_tab, y_in_tab, x_in_tab, val_energy_in, cond_energy_in, occupation_in, out,
    val_energy, cond_energy, occupation, gvec, z_tab, y_tab, x_tab, vbuf, cbuf, wide, tab, mixed, sec, keys,
    parts, core_in, z_out, z_in, cols, rows, left, sums, far_out, far_in, x_out, x_in,
    small_sems, load_sems, core_sems, z_sems, zh_sems, y_sems, row_sems, far_sems, x_sems, out_sems,
):
    y, x, zl, core, zh = (lax.axis_index(a) for a in MESH_AXES)
    grow = 2 * zl + core
    loads = [
        [pltpu.make_async_copy(a.at[pl.ds(3 * s, 3)], b.at[pl.ds(3 * s, 3)], load_sems.at[i, s]) for i, (a, b) in enumerate([(val, vbuf), (con, cbuf)])]
        for s in range(4)
    ]
    small = [
        pltpu.make_async_copy(a, b, small_sems.at[i])
        for i, (a, b) in enumerate([
            (gvec_in, gvec), (z_in_tab, z_tab), (y_in_tab, y_tab), (x_in_tab.at[grow], x_tab),
            (val_energy_in, val_energy), (cond_energy_in, cond_energy), (occupation_in, occupation),
        ])
    ]
    for c in small[:1] + [c for pair in loads for c in pair] + small[1:]:
        c.start()

    barrier = pltpu.get_barrier_semaphore()
    other = {"core": 1 - core}
    partners = [other] + [{"zl": turned("zl", k)} for k in (1, 2, 3)] + [{"zh": turned("zh", k)} for k in (1, 2)]
    partners += [{"y": turned("y", k)} for k in (1, 7)] + [{"x": turned("x", k)} for k in (1, 3)]
    for target in partners:
        pl.semaphore_signal(barrier, inc=1, device_id=target, device_id_type=SIDE)

    with scope("keys"):
        small[0].wait()
        build_keys(gvec, keys)
    with scope("mix"):
        for s in range(4):
            for c in loads[s]:
                c.wait()
            mix_planes(3 * s, 3 * s + 3, vbuf, cbuf, wide, mixed)
    for c in small[1:]:
        c.wait()
    with scope("planes"):
        build_waves(0, z_tab, y_tab, tab)
        for t in range(4):
            if t < 3:
                build_waves(t + 1, z_tab, y_tab, tab)
            plane_sums(t, mixed, tab, sec)
        factor = pair_factor(val_energy[...], cond_energy[...], occupation[...])
    with scope("barrier"):
        pl.semaphore_wait(barrier, len(partners))

    odd = 1 - lax.rem(zl, 2)

    def swap(k, q):
        return remote(parts.at[turned("zl", k), 1 - core, q], core_in.at[q, k], out_sems.at[0], core_sems.at[q], other)

    def pass_on(k, q):
        return remote(z_out.at[q, k - 1], z_in.at[q, k - 1], out_sems.at[1], z_sems.at[q], {"zl": turned("zl", k)})

    def both_cores(k, q):
        return parts[turned("zl", k), core, q].astype(jnp.float32) + core_in[q, k].astype(jnp.float32)

    def combine(q):
        remote(core_in.at[q], core_in.at[q], out_sems.at[0], core_sems.at[q], other).wait_recv()
        for k in (2, 1, 3):
            z_out[q, k - 1] = both_cores(k, q).astype(jnp.bfloat16)
            pass_on(k, q).start()

    for q in range(4):
        with scope("pick%d" % q):
            for block in (2 * odd + 1 - core, 3 - core - 2 * odd, 2 * odd + core, 2 - 2 * odd + core):
                pick(block, q, parts, x_tab, sec, keys)
            for k in (1, 3, 2, 0):
                swap(k, q).start()
        if q:
            with scope("combine%d" % (q - 1)):
                combine(q - 1)
    with scope("combine3"):
        combine(3)

    home = y // 2
    on_chain = core == lax.rem(y, 2)
    source = on_chain & (zl == home)

    def row_copy(s, i, target):
        return remote(rows.at[s], rows.at[s], out_sems.at[6 + i], row_sems.at[s], target)

    def along(s, first):
        @pl.when((zl < 3) & ((zl > home) | first))
        def _():
            row_copy(s, 1, {"zl": turned("zl", 1)}).start()

        @pl.when((zl > 0) & ((zl < home) | first))
        def _():
            row_copy(s, 2, {"zl": turned("zl", 3)}).start()

    def rows_here(first, last):
        @pl.when(jnp.logical_not(on_chain))
        def _():
            for s in range(first, last):
                row_copy(s, 0, other).wait_recv()

    def through(q):
        return remote(far_out.at[q], far_in.at[q], out_sems.at[4], far_sems.at[q], {"x": turned("x", 1 if q < 2 else 3)})

    def send_sum(side, q):
        return remote(x_out.at[side, q], x_in.at[side, q], out_sems.at[5], x_sems.at[side, q], {"x": turned("x", 3 if side else 1)})

    def group_of(k, q):
        return sums[q, pl.ds(pl.multiple_of(80 * turned("x", k), 80), 80)]

    def product(q, first, last):
        pairs = slice(32 * first, 32 * last)
        right = cols[q // 2, first:last, :, SUB * (q % 2) : SUB * (q % 2 + 1)].reshape(32 * (last - first), SUB)
        return jnp.dot(left[:, pairs], right, preferred_element_type=jnp.float32)

    def turn(first, last):
        left[:, 32 * first : 32 * last] = rows[first:last, :, 0:320].reshape(32 * (last - first), 320).T

    def gather(third):
        order, slot = TABLES[third]

        def to_gcol(k, h):
            return remote(cols.at[h, slot[0, 0]], cols.at[h, TABLES[(third + k) % 3][1][k, 0]], out_sems.at[2], zh_sems.at[k - 1, h], {"zh": turned("zh", k)})

        def ring(t, way, hop, h):
            held = slot[t, step_of(way, hop - 1) if hop > 1 else 0]
            return remote(cols.at[h, held], cols.at[h, slot[t, step_of(way, hop)]], out_sems.at[3], y_sems.at[RING_AT[t, way, hop, h]], {"y": turned("y", way)})

        def give(t, step):
            s = slot[t, step]

            @pl.when(source)
            def _():
                for q in range(4):
                    at = SUB * (q % 2) + 80 * third
                    rows[s, :, 80 * q : 80 * q + 80] = cols[q // 2, s, :, at : at + 80]

                if s < CHAINED:
                    along(s, True)
                else:
                    for k in (3, 2, 1):
                        row_copy(s, 3, {"zl": turned("zl", k)}).start()
                row_copy(s, 0, other).start()

        def relay(t, step, far):
            s = slot[t, step]
            away = (zl != home) if s >= CHAINED else ((zl == home + far) | (zl == home - far))

            @pl.when(on_chain & away)
            def _():
                row_copy(s, 0, other).wait_recv()
                if s < CHAINED and far < 3:
                    along(s, False)
                row_copy(s, 0, other).start()

        def handle(event):
            kind = event[0]
            if kind == "own":
                h = event[1]
                with scope("own%d" % h):
                    for q in (2 * h, 2 * h + 1):
                        remote(z_in.at[q], z_in.at[q], out_sems.at[1], z_sems.at[q], other).wait_recv()
                        total = both_cores(0, q)
                        for k in range(3):
                            total += z_in[q, k].astype(jnp.float32)
                        cols[h, slot[0, 0], :, SUB * (q % 2) : SUB * (q % 2 + 1)] = (total * factor).astype(jnp.bfloat16)
                for k in (1, 2):
                    to_gcol(k, h).start()
                for way in (1, -1):
                    ring(0, way, 1, h).start()
            elif kind == "zh":
                _, t, h = event
                with scope("zh%d%d" % (t, h)):
                    to_gcol(t, h).wait_recv()
                for way in (1, -1):
                    ring(t, way, 1, h).start()
            elif kind == "ring":
                _, t, way, hop, h = event
                with scope("ring%d%d%d%d" % (t, max(way, 0), hop, h)):
                    ring(t, way, hop, h).wait_recv()
                if hop < 4 and h in carried(way, hop + 1):
                    ring(t, way, hop + 1, h).start()
            elif kind == "give":
                give(*event[1:])
            else:
                relay(*event[1:])

        until = max(i for i, event in enumerate(order) if event[0] == "relay" and slot[event[1:3]] < EARLY) + 1
        for event in order[:until]:
            handle(event)
        with scope("early"):
            rows_here(0, EARLY)
            turn(0, EARLY)
            for q in range(4):
                sums[q] = product(q, 0, EARLY)
        for event in order[until:]:
            handle(event)

    for third in range(3):

        @pl.when(zh == third)
        def _():
            gather(third)

    with scope("rows"):
        rows_here(EARLY, 24)
    with scope("matmul"):
        turn(EARLY, 24)
        for q in range(4):
            sums[q] = sums[q] + product(q, EARLY, 24)
            far_out[q] = group_of(2, q).astype(jnp.bfloat16)
            through(q).start()
            side = 1 if q < 2 else 0
            x_out[side, q] = group_of(3 if side else 1, q).astype(jnp.bfloat16)
            send_sum(side, q).start()
    with scope("xpass"):
        for q in (0, 2, 1, 3):
            side = 0 if q < 2 else 1
            through(q).wait_recv()
            x_out[side, q] = (group_of(3 if side else 1, q) + far_in[q].astype(jnp.float32)).astype(jnp.bfloat16)
            send_sum(side, q).start()
    for q in (0, 2, 1, 3):
        with scope("xsum%d" % q):
            total = group_of(0, q)
            for side in ((1, 0) if q < 2 else (0, 1)):
                send_sum(side, q).wait_recv()
                total += x_in[side, q].astype(jnp.float32)
            out[:, QUARTER * q : QUARTER * (q + 1)] = total[:, :QUARTER]

    def gone(ref, i):
        remote(ref, ref, out_sems.at[i], far_sems.at[0], other).wait_send()

    with scope("gone"):
        gone(core_in, 0)
        gone(z_in, 1)
        gone(cols.at[:, 0:2], 2)
        gone(cols.at[:, 0:21], 3)
        gone(far_in, 4)
        gone(x_in, 5)

        @pl.when(on_chain)
        def _():
            gone(rows, 6)

        @pl.when(on_chain & (zl < 3) & (zl >= home))
        def _():
            gone(rows.at[0:CHAINED], 7)

        @pl.when(on_chain & (zl > 0) & (zl <= home))
        def _():
            gone(rows.at[0:CHAINED], 8)

        @pl.when(source)
        def _():
            gone(rows.at[0 : 3 * (24 - CHAINED)], 9)


def scratch():
    dma = pltpu.SemaphoreType.DMA
    bf = jnp.bfloat16
    f32 = jnp.float32
    return [
        pltpu.VMEM((1, NV), f32), pltpu.VMEM((1, 192), f32), pltpu.VMEM((1, NV), jnp.int32),
        pltpu.VMEM((3, KG), jnp.int32), pltpu.VMEM((2, 2, N, 128), f32), pltpu.VMEM((5, 2, 12, 128), f32), pltpu.VMEM((32, 16), bf),
        pltpu.VMEM((PLANES, NV, N * N), bf), pltpu.VMEM((PLANES, 2, N * N), bf), pltpu.VMEM((PLANES, 2, N * N), f32),
        pltpu.VMEM((4, 2 * PART, 256), bf), pltpu.VMEM((4, 384, 2 * PART), bf), pltpu.VMEM((PLANES, 2, 32, 512), bf), pltpu.VMEM((4, 8, 4 * SUB), jnp.int32),
        pltpu.VMEM((4, 2, 4, 32, SUB), bf), pltpu.VMEM((4, 4, 32, SUB), bf), pltpu.VMEM((4, 3, 32, SUB), bf), pltpu.VMEM((4, 3, 32, SUB), bf),
        pltpu.VMEM((2, 24, 32, 2 * SUB), bf), pltpu.VMEM((24, 32, 384), bf), pltpu.VMEM((320, 768), bf), pltpu.VMEM((4, 320, SUB), f32), pltpu.VMEM((4, 80, SUB), bf), pltpu.VMEM((4, 80, SUB), bf), pltpu.VMEM((2, 4, 80, SUB), bf), pltpu.VMEM((2, 4, 80, SUB), bf),
        dma((7,)), dma((2, 4)), dma((4,)), dma((4,)), dma((2, 2)), dma((len(RING),)), dma((24,)), dma((4,)), dma((2, 4)), dma((10,)),
    ]


def body(valence, conduction, val_energy, cond_energy, val_occupation, gvectors):
    z_tab, y_tab, x_tab = tables()
    chi = pl.pallas_call(
        chi_body,
        out_shape=pltpu.VMEM((80, 4 * QUARTER), jnp.float32),
        in_specs=[pl.BlockSpec(memory_space=pl.ANY)] * 9,
        out_specs=pl.BlockSpec(memory_space=pltpu.VMEM),
        scratch_shapes=scratch(),
        compiler_params=pltpu.CompilerParams(collective_id=0, has_side_effects=True, vmem_limit_bytes=60 * 2**20),
        name="chi",
    )(
        valence.transpose(1, 0, 2), conduction.transpose(1, 0, 2), gvectors,
        jnp.asarray(z_tab), jnp.asarray(y_tab), jnp.asarray(x_tab, jnp.bfloat16),
        val_energy.reshape(1, NV), cond_energy.reshape(1, 192), val_occupation.reshape(1, NV),
    )
    return chi * (-1.0 / math.sqrt(3072))


def solution(mesh):
    finer = Mesh(mesh.devices.reshape(8, 4, 4, 2, 3), MESH_AXES)
    grow = ("zl", "core")
    bands = ("y", "x", "zh")
    placed = (P(None, grow, None), P(bands, grow, None), P(), P(), P(), P())
    return jax.shard_map(body, mesh=finer, in_specs=placed, out_specs=P(bands, grow), check_vma=False)
```
